32 devices in a mesh: dp: 8 (over y, x, core), tensor: 4 (over z).
Axes of the slice: x: 2, y: 2, z: 4, core: 2. Of those that a mesh axis runs over, the one named last changes fastest.
Arguments:
- images: bfloat16 [8, 577, 1024], P('dp'), may hold values from -6 to 6
- valid_flags: int32 [8], P('dp'), may hold values from 0 to 1, as said below
- cotangent: bfloat16 [8, 577, 1024], P('dp'), may hold values from -6 to 6
- first_gain: float32 [1024], P('dp'), may hold values from 0.5 to 1.5
- first_shift: float32 [1024], P('dp'), may hold values from -1.75 to 1.75
- triple_weight: float32 [3, 1024, 1024], P(None, 'dp', 'tensor'), may hold values from -0.1875 to 0.1875
- pair_bias: float32 [2, 16, 64], P(None, 'tensor', 'dp'), may hold values from -1.75 to 1.75
- output_weight: float32 [1024, 1024], P('tensor', 'dp'), may hold values from -1.5 to 1.5
- output_bias: float32 [1024], P('dp'), may hold values from -1.75 to 1.75
- second_gain: float32 [1024], P('dp'), may hold values from 0.5 to 1.5
- second_shift: float32 [1024], P('dp'), may hold values from -1.75 to 1.75
- expand_weight: float32 [1024, 4096], P('dp', 'tensor'), may hold values from -1 to 1, as said below
- expand_bias: float32 [64, 64], P('tensor', 'dp'), may hold values from -1.75 to 1.75
- reduce_weight: float32 [4096, 1024], P('tensor', 'dp'), may hold values from -1 to 1, as said below
- reduce_bias: float32 [1024], P('dp'), may hold values from -1.75 to 1.75
- first_gain_mean: float32 [1024], P('dp'), may hold values from -6 to 6
- first_shift_mean: float32 [1024], P('dp'), may hold values from -6 to 6
- triple_weight_mean: float32 [3, 1024, 1024], P(None, 'dp', 'tensor'), may hold values from -6 to 6
- pair_bias_mean: float32 [2, 16, 64], P(None, 'tensor', 'dp'), may hold values from -6 to 6
- output_weight_mean: float32 [1024, 1024], P('tensor', 'dp'), may hold values from -6 to 6
- output_bias_mean: float32 [1024], P('dp'), may hold values from -6 to 6
- second_gain_mean: float32 [1024], P('dp'), may hold values from -6 to 6
- second_shift_mean: float32 [1024], P('dp'), may hold values from -6 to 6
- expand_weight_mean: float32 [1024, 4096], P('dp', 'tensor'), may hold values from -6 to 6
- expand_bias_mean: float32 [64, 64], P('tensor', 'dp'), may hold values from -6 to 6
- reduce_weight_mean: float32 [4096, 1024], P('tensor', 'dp'), may hold values from -6 to 6
- reduce_bias_mean: float32 [1024], P('dp'), may hold values from -6 to 6
- first_gain_square: float32 [1024], P('dp'), may hold values from 1 to 4
- first_shift_square: float32 [1024], P('dp'), may hold values from 1 to 4
- triple_weight_square: float32 [3, 1024, 1024], P(None, 'dp', 'tensor'), may hold values from 1 to 4
- pair_bias_square: float32 [2, 16, 64], P(None, 'tensor', 'dp'), may hold values from 1 to 4
- output_weight_square: float32 [1024, 1024], P('tensor', 'dp'), may hold values from 1 to 4
- output_bias_square: float32 [1024], P('dp'), may hold values from 1 to 4
- second_gain_square: float32 [1024], P('dp'), may hold values from 1 to 4
- second_shift_square: float32 [1024], P('dp'), may hold values from 1 to 4
- expand_weight_square: float32 [1024, 4096], P('dp', 'tensor'), may hold values from 1 to 4
- expand_bias_square: float32 [64, 64], P('tensor', 'dp'), may hold values from 1 to 4
- reduce_weight_square: float32 [4096, 1024], P('tensor', 'dp'), may hold values from 1 to 4
- reduce_bias_square: float32 [1024], P('dp'), may hold values from 1 to 4
Outputs:
- block_output: bfloat16 [8, 577, 1024], P('dp')
- input_grad: float32 [8, 577, 1024], P('dp')
- grad_norm: float32 [], replicated
- new_first_gain: float32 [1024], P('dp')
- mean_first_gain: float32 [1024], P('dp')
- square_first_gain: float32 [1024], P('dp')
- copy_first_gain: bfloat16 [1024], P('dp')
- new_first_shift: float32 [1024], P('dp')
- mean_first_shift: float32 [1024], P('dp')
- square_first_shift: float32 [1024], P('dp')
- copy_first_shift: bfloat16 [1024], P('dp')
- new_triple_weight: float32 [3, 1024, 1024], P(None, 'dp', 'tensor')
- mean_triple_weight: float32 [3, 1024, 1024], P(None, 'dp', 'tensor')
- square_triple_weight: float32 [3, 1024, 1024], P(None, 'dp', 'tensor')
- copy_triple_weight: bfloat16 [3, 1024, 1024], P(None, 'dp', 'tensor')
- new_pair_bias: float32 [2, 16, 64], P(None, 'tensor', 'dp')
- mean_pair_bias: float32 [2, 16, 64], P(None, 'tensor', 'dp')
- square_pair_bias: float32 [2, 16, 64], P(None, 'tensor', 'dp')
- copy_pair_bias: bfloat16 [2, 16, 64], P(None, 'tensor', 'dp')
- new_output_weight: float32 [1024, 1024], P('tensor', 'dp')
- mean_output_weight: float32 [1024, 1024], P('tensor', 'dp')
- square_output_weight: float32 [1024, 1024], P('tensor', 'dp')
- copy_output_weight: bfloat16 [1024, 1024], P('tensor', 'dp')
- new_output_bias: float32 [1024], P('dp')
- mean_output_bias: float32 [1024], P('dp')
- square_output_bias: float32 [1024], P('dp')
- copy_output_bias: bfloat16 [1024], P('dp')
- new_second_gain: float32 [1024], P('dp')
- mean_second_gain: float32 [1024], P('dp')
- square_second_gain: float32 [1024], P('dp')
- copy_second_gain: bfloat16 [1024], P('dp')
- new_second_shift: float32 [1024], P('dp')
- mean_second_shift: float32 [1024], P('dp')
- square_second_shift: float32 [1024], P('dp')
- copy_second_shift: bfloat16 [1024], P('dp')
- new_expand_weight: float32 [1024, 4096], P('dp', 'tensor')
- mean_expand_weight: float32 [1024, 4096], P('dp', 'tensor')
- square_expand_weight: float32 [1024, 4096], P('dp', 'tensor')
- copy_expand_weight: bfloat16 [1024, 4096], P('dp', 'tensor')
- new_expand_bias: float32 [64, 64], P('tensor', 'dp')
- mean_expand_bias: float32 [64, 64], P('tensor', 'dp')
- square_expand_bias: float32 [64, 64], P('tensor', 'dp')
- copy_expand_bias: bfloat16 [64, 64], P('tensor', 'dp')
- new_reduce_weight: float32 [4096, 1024], P('tensor', 'dp')
- mean_reduce_weight: float32 [4096, 1024], P('tensor', 'dp')
- square_reduce_weight: float32 [4096, 1024], P('tensor', 'dp')
- copy_reduce_weight: bfloat16 [4096, 1024], P('tensor', 'dp')
- new_reduce_bias: float32 [1024], P('dp')
- mean_reduce_bias: float32 [1024], P('dp')
- square_reduce_bias: float32 [1024], P('dp')
- copy_reduce_bias: bfloat16 [1024], P('dp')
The draws below stay inside these ranges and needn't reach their ends.
Inputs may be any that keep to these rules, and one draw needn't show every extreme that they name: `valid_flags`: at least one image is blank; blank images may stand anywhere in the batch. `expand_weight`: a projection matrix with entries of order one over the root of 1024. `reduce_weight`: a projection matrix with entries of order one over the root of 4096.
All inputs are finite; a program needn't handle non-finite values.
Results may differ from the reference program's by a relative error of at most 0.012.
The reference program's roundings to bfloat16 on the way count: a program that leaves them out, or rounds other values in their place, can miss the bound.
Values may be sent and summed in bfloat16 or wider, within the bound.
A program may use at most 128 MiB of HBM per device.

```python
import math
import jax
import jax.numpy as jnp
from jax import lax

D = 1024
HEADS = 16
HD = 64
FF = 4096
SEQ = 577
IMAGES = 8


def draw_valid_flags(key, part):
    level = jax.random.randint(jax.random.fold_in(key, 11), (IMAGES,), 0, 8)
    blank_place = jax.random.randint(jax.random.fold_in(key, 23), (), 0, IMAGES)
    places = jnp.arange(IMAGES, dtype=jnp.int32)
    flags = (level > 0).astype(jnp.int32)
    return jnp.where(places == blank_place, 0, flags).astype(jnp.int32)


def unit_profile(count):
    ratio = 3.0
    where = jnp.arange(count, dtype=jnp.float32) / float(max(count - 1, 1))
    return jnp.exp(jnp.log(ratio) * (where - 0.5))


def draw_expand_weight(key, part):
    noise = jnp.clip(jax.random.normal(jax.random.fold_in(key, 31), (D, FF), jnp.float32), -6.0, 6.0)
    return noise * D ** (-0.5) * unit_profile(FF)[None, :]


def draw_reduce_weight(key, part):
    noise = jnp.clip(jax.random.normal(jax.random.fold_in(key, 37), (FF, D), jnp.float32), -6.0, 6.0)
    return noise * FF ** (-0.5) * unit_profile(FF)[:, None]


def block_scale(rng, dims, cuts, low, top_value):
    def one(position, blocks):
        steps = jax.random.uniform(jax.random.fold_in(jax.random.fold_in(rng, 6), position), (blocks,), jnp.float32, low / len(cuts), top_value / len(cuts))
        return jnp.repeat(jnp.exp(steps), dims[position] // blocks).reshape((-1,) + (1,) * (len(dims) - position - 1))

    level = one(*cuts[0])
    for cut in cuts[1:]:
        level = level * one(*cut)
    return level


def normal_values(own_key, dims, width, most, pieces=(), held_as=jnp.bfloat16):
    values = width * jax.random.normal(own_key, dims, jnp.float32)
    if pieces:
        values = values * block_scale(own_key, dims, pieces, -0.22, 0.18)
    return jnp.clip(values, -most, most).astype(held_as)


def setup_inputs(seed: int = 0) -> dict:
    key_list = jax.random.split(jax.random.key(seed), 40)
    images = normal_values(key_list[0], (IMAGES, SEQ, D), 1.0, 6.0, ((0, 8),))
    valid_flags = draw_valid_flags(jax.random.fold_in(key_list[39], 71), 0)
    cotangent = normal_values(key_list[2], (IMAGES, SEQ, D), 1.0, 6.0, ((0, 8),))
    first_gain = jnp.clip(1.0 + 0.1 * jax.random.normal(key_list[3], (D,), jnp.float32), 0.5, 1.5)
    first_shift = normal_values(key_list[4], (D,), 0.3, 1.75, ((0, 8),), jnp.float32)
    triple_weight = normal_values(key_list[5], (3, D, D), D ** -0.5, 0.1875, ((1, 8), (2, 4)), jnp.float32)
    pair_bias = normal_values(key_list[6], (2, HEADS, HD), 0.3, 1.75, ((1, 4), (2, 8)), jnp.float32)
    output_weight = normal_values(key_list[7], (D, D), (max(1, 8 * D // SEQ)) ** -0.5, 1.5, ((0, 4), (1, 8)), jnp.float32)
    output_bias = normal_values(key_list[8], (D,), 0.3, 1.75, ((0, 8),), jnp.float32)
    second_gain = jnp.clip(1.0 + 0.1 * jax.random.normal(key_list[9], (D,), jnp.float32), 0.5, 1.5)
    second_shift = normal_values(key_list[10], (D,), 0.3, 1.75, ((0, 8),), jnp.float32)
    expand_weight = draw_expand_weight(jax.random.fold_in(key_list[39], 71), 0)
    expand_bias = normal_values(key_list[12], (FF // HD, HD), 0.3, 1.75, ((0, 4), (1, 8)), jnp.float32)
    reduce_weight = draw_reduce_weight(jax.random.fold_in(key_list[39], 71), 0)
    reduce_bias = normal_values(key_list[14], (D,), 0.3, 1.75, ((0, 8),), jnp.float32)
    first_gain_mean = normal_values(key_list[15], (D,), 1.0, 6.0, ((0, 8),), jnp.float32)
    first_shift_mean = normal_values(key_list[16], (D,), 1.0, 6.0, ((0, 8),), jnp.float32)
    triple_weight_mean = normal_values(key_list[17], (3, D, D), 1.0, 6.0, ((1, 8), (2, 4)), jnp.float32)
    pair_bias_mean = normal_values(key_list[18], (2, HEADS, HD), 1.0, 6.0, ((1, 4), (2, 8)), jnp.float32)
    output_weight_mean = normal_values(key_list[19], (D, D), 1.0, 6.0, ((0, 4), (1, 8)), jnp.float32)
    output_bias_mean = normal_values(key_list[20], (D,), 1.0, 6.0, ((0, 8),), jnp.float32)
    second_gain_mean = normal_values(key_list[21], (D,), 1.0, 6.0, ((0, 8),), jnp.float32)
    second_shift_mean = normal_values(key_list[22], (D,), 1.0, 6.0, ((0, 8),), jnp.float32)
    expand_weight_mean = normal_values(key_list[23], (D, FF), 1.0, 6.0, ((0, 8), (1, 4)), jnp.float32)
    expand_bias_mean = normal_values(key_list[24], (FF // HD, HD), 1.0, 6.0, ((0, 4), (1, 8)), jnp.float32)
    reduce_weight_mean = normal_values(key_list[25], (FF, D), 1.0, 6.0, ((0, 4), (1, 8)), jnp.float32)
    reduce_bias_mean = normal_values(key_list[26], (D,), 1.0, 6.0, ((0, 8),), jnp.float32)
    first_gain_square = jnp.clip(jnp.exp(math.log(4.0) - 1.3862944 * jax.random.uniform(key_list[27], (D,), jnp.float32) ** block_scale(key_list[27], (D,), ((0, 8),), -0.2, 0.2)), 1.0, 4.0)
    first_shift_square = jnp.clip(jnp.exp(math.log(4.0) - 1.3862944 * jax.random.uniform(key_list[28], (D,), jnp.float32) ** block_scale(key_list[28], (D,), ((0, 8),), -0.2, 0.2)), 1.0, 4.0)
    triple_weight_square = jnp.clip(jnp.exp(math.log(4.0) - 1.3862944 * jax.random.uniform(key_list[29], (3, D, D), jnp.float32) ** block_scale(key_list[29], (3, D, D), ((1, 8), (2, 4)), -0.2, 0.2)), 1.0, 4.0)
    pair_bias_square = jnp.clip(jnp.exp(math.log(4.0) - 1.3862944 * jax.random.uniform(key_list[30], (2, HEADS, HD), jnp.float32) ** block_scale(key_list[30], (2, HEADS, HD), ((1, 4), (2, 8)), -0.2, 0.2)), 1.0, 4.0)
    output_weight_square = jnp.clip(jnp.exp(math.log(4.0) - 1.3862944 * jax.random.uniform(key_list[31], (D, D), jnp.float32) ** block_scale(key_list[31], (D, D), ((0, 4), (1, 8)), -0.2, 0.2)), 1.0, 4.0)
    output_bias_square = jnp.clip(jnp.exp(math.log(4.0) - 1.3862944 * jax.random.uniform(key_list[32], (D,), jnp.float32) ** block_scale(key_list[32], (D,), ((0, 8),), -0.2, 0.2)), 1.0, 4.0)
    second_gain_square = jnp.clip(jnp.exp(math.log(4.0) - 1.3862944 * jax.random.uniform(key_list[33], (D,), jnp.float32) ** block_scale(key_list[33], (D,), ((0, 8),), -0.2, 0.2)), 1.0, 4.0)
    second_shift_square = jnp.clip(jnp.exp(math.log(4.0) - 1.3862944 * jax.random.uniform(key_list[34], (D,), jnp.float32) ** block_scale(key_list[34], (D,), ((0, 8),), -0.2, 0.2)), 1.0, 4.0)
    expand_weight_square = jnp.clip(jnp.exp(math.log(4.0) - 1.3862944 * jax.random.uniform(key_list[35], (D, FF), jnp.float32) ** block_scale(key_list[35], (D, FF), ((0, 8), (1, 4)), -0.2, 0.2)), 1.0, 4.0)
    expand_bias_square = jnp.clip(jnp.exp(math.log(4.0) - 1.3862944 * jax.random.uniform(key_list[36], (FF // HD, HD), jnp.float32) ** block_scale(key_list[36], (FF // HD, HD), ((0, 4), (1, 8)), -0.2, 0.2)), 1.0, 4.0)
    reduce_weight_square = jnp.clip(jnp.exp(math.log(4.0) - 1.3862944 * jax.random.uniform(key_list[37], (FF, D), jnp.float32) ** block_scale(key_list[37], (FF, D), ((0, 4), (1, 8)), -0.2, 0.2)), 1.0, 4.0)
    reduce_bias_square = jnp.clip(jnp.exp(math.log(4.0) - 1.3862944 * jax.random.uniform(key_list[38], (D,), jnp.float32) ** block_scale(key_list[38], (D,), ((0, 8),), -0.2, 0.2)), 1.0, 4.0)
    return {"images": images, "valid_flags": valid_flags, "cotangent": cotangent, "first_gain": first_gain, "first_shift": first_shift, "triple_weight": triple_weight, "pair_bias": pair_bias, "output_weight": output_weight, "output_bias": output_bias, "second_gain": second_gain, "second_shift": second_shift, "expand_weight": expand_weight, "expand_bias": expand_bias, "reduce_weight": reduce_weight, "reduce_bias": reduce_bias, "first_gain_mean": first_gain_mean, "first_shift_mean": first_shift_mean, "triple_weight_mean": triple_weight_mean, "pair_bias_mean": pair_bias_mean, "output_weight_mean": output_weight_mean, "output_bias_mean": output_bias_mean, "second_gain_mean": second_gain_mean, "second_shift_mean": second_shift_mean, "expand_weight_mean": expand_weight_mean, "expand_bias_mean": expand_bias_mean, "reduce_weight_mean": reduce_weight_mean, "reduce_bias_mean": reduce_bias_mean, "first_gain_square": first_gain_square, "first_shift_square": first_shift_square, "triple_weight_square": triple_weight_square, "pair_bias_square": pair_bias_square, "output_weight_square": output_weight_square, "output_bias_square": output_bias_square, "second_gain_square": second_gain_square, "second_shift_square": second_shift_square, "expand_weight_square": expand_weight_square, "expand_bias_square": expand_bias_square, "reduce_weight_square": reduce_weight_square, "reduce_bias_square": reduce_bias_square}


@jax.custom_vjp
def low(v):
    return lax.optimization_barrier(v.astype(jnp.bfloat16)).astype(jnp.float32)

@jax.custom_vjp
def low_back(v):
    return v

def low_keep(v):
    return (low(v), None)

def low_pass(kept, grad):
    return (grad,)

def back_keep(v):
    return (v, None)

def back_low(kept, grad):
    return (low(grad),)
low.defvjp(low_keep, low_pass)
low_back.defvjp(back_keep, back_low)
rates = (0.2, 0.2, 0.03, 0.2, 0.03, 0.2, 0.2, 0.2, 0.03, 0.2, 0.03, 0.2)

def both_ways(value):
    return low_back(low(value))

def mult(left, right):
    return jnp.dot(left, right, precision=lax.Precision.HIGHEST, preferred_element_type=jnp.float32)

def apply_layer_norm(input_row_block, norm_gain, norm_bias):
    center = lax.optimization_barrier(jnp.mean(input_row_block, axis=-1, keepdims=True))
    centered_rows = input_row_block - center
    spread = lax.optimization_barrier(jnp.mean(centered_rows * centered_rows, axis=-1, keepdims=True))
    return centered_rows * lax.rsqrt(spread + 1e-06) * norm_gain + norm_bias

def attend(parts):
    query, keys, values = parts
    scores = jnp.einsum('hqd,hkd->hqk', query, keys, precision=lax.Precision.HIGHEST) * HD ** (-0.5)
    scores = low_back(scores)
    top = lax.optimization_barrier(jnp.max(scores, axis=-1, keepdims=True))
    weights = jnp.exp(scores - top)
    probs = weights / lax.optimization_barrier(jnp.sum(weights, axis=-1, keepdims=True))
    return jnp.einsum('hqk,hkd->hqd', low(probs), values, precision=lax.Precision.HIGHEST)

def forward(input_row_block, params):
    gain_first, shift_first, triple, pairs, out_weight, out_bias, gain_second, shift_second, up_weight, up_bias, down_weight, down_bias = [low(p) for p in params]
    flat = input_row_block.reshape(IMAGES * SEQ, D)
    first = low(apply_layer_norm(flat, gain_first, shift_first))
    pairs_flat = pairs.reshape(2, D)
    query = both_ways(mult(first, triple[0]) + pairs_flat[0])
    keys = both_ways(mult(first, triple[1]))
    values = both_ways(mult(first, triple[2]) + pairs_flat[1])

    def by_heads(block):
        return block.reshape(IMAGES, SEQ, HEADS, HD).transpose(0, 2, 1, 3)
    mixed = lax.map(jax.checkpoint(attend), (by_heads(query), by_heads(keys), by_heads(values)))
    mixed = both_ways(mixed.transpose(0, 2, 1, 3).reshape(IMAGES * SEQ, D))
    middle_state = flat + low_back(mult(mixed, out_weight)) + out_bias
    second = low(apply_layer_norm(middle_state, gain_second, shift_second))
    hidden = low_back(mult(second, up_weight)) + up_bias.reshape(FF)
    active = low(jax.nn.gelu(hidden, approximate=False))
    result = middle_state + low_back(mult(active, down_weight)) + down_bias
    return result.reshape(IMAGES, SEQ, D)

def adam_step(master, row_mean, square, incoming_gradient, rate):
    mean_new = 0.5 * row_mean + 0.5 * incoming_gradient
    square_new = 0.5 * square + 0.5 * incoming_gradient * incoming_gradient
    change = -rate * (mean_new / (jnp.sqrt(square_new) + 1e-08) + 0.1 * master)
    updated = master + change
    return [updated, mean_new, square_new, updated.astype(jnp.bfloat16)]

def reference(images, valid_flags, cotangent, first_gain, first_shift, triple_weight, pair_bias, output_weight, output_bias, second_gain, second_shift, expand_weight, expand_bias, reduce_weight, reduce_bias, first_gain_mean, first_shift_mean, triple_weight_mean, pair_bias_mean, output_weight_mean, output_bias_mean, second_gain_mean, second_shift_mean, expand_weight_mean, expand_bias_mean, reduce_weight_mean, reduce_bias_mean, first_gain_square, first_shift_square, triple_weight_square, pair_bias_square, output_weight_square, output_bias_square, second_gain_square, second_shift_square, expand_weight_square, expand_bias_square, reduce_weight_square, reduce_bias_square):
    masters = (first_gain, first_shift, triple_weight, pair_bias, output_weight, output_bias, second_gain, second_shift, expand_weight, expand_bias, reduce_weight, reduce_bias)
    means = (first_gain_mean, first_shift_mean, triple_weight_mean, pair_bias_mean, output_weight_mean, output_bias_mean, second_gain_mean, second_shift_mean, expand_weight_mean, expand_bias_mean, reduce_weight_mean, reduce_bias_mean)
    squares = (first_gain_square, first_shift_square, triple_weight_square, pair_bias_square, output_weight_square, output_bias_square, second_gain_square, second_shift_square, expand_weight_square, expand_bias_square, reduce_weight_square, reduce_bias_square)
    input_row_block = images.astype(jnp.float32)
    result, pullback = jax.vjp(forward, input_row_block, masters)
    scaled_rows = cotangent.astype(jnp.float32) * valid_flags.astype(jnp.float32)[:, None, None]
    row_gradient, grads = pullback(scaled_rows)
    total = jnp.zeros((), jnp.float32)
    for incoming_gradient in grads:
        total = total + jnp.sum(incoming_gradient * incoming_gradient)
    norm_value = jnp.sqrt(total)
    limit = math.sqrt(4 * D * D + 2 * D * FF + 8 * D + FF)
    factor = jnp.minimum(1.0, limit / (norm_value + 1e-06))
    updates = []
    for master, row_mean, square, incoming_gradient, rate in zip(masters, means, squares, grads, rates):
        updates.extend(adam_step(master, row_mean, square, incoming_gradient * factor, rate))
    return (result.astype(jnp.bfloat16), row_gradient, norm_value, *updates)
```

```python
import functools
import math
import types

import jax
import jax.numpy as jnp
from jax import lax
from jax.experimental import pallas as pl
from jax.experimental.pallas import tpu as pltpu
from jax.sharding import PartitionSpec as P

D = 1024
FF = 4096


shard_dims = (0, 0, 1, 2, 1, 0, 0, 0, 0, 1, 1, 0)
shared_terms = (1, 1, 0, 0, 0, 1, 1, 1, 0, 0, 0, 1)
rates = (0.2, 0.2, 0.03, 0.2, 0.03, 0.2, 0.2, 0.2, 0.03, 0.2, 0.03, 0.2)


def apply_layer_norm(input_row_block, norm_gain, norm_bias):
    center = jnp.mean(input_row_block, axis=-1, keepdims=True)
    centered_rows = input_row_block - center
    inverse_deviation = lax.rsqrt(
        jnp.mean(centered_rows * centered_rows, axis=-1, keepdims=True) + 1e-06
    )
    standardized_rows = centered_rows * inverse_deviation
    return (
        standardized_rows * norm_gain.astype(jnp.float32) + norm_bias.astype(jnp.float32),
        standardized_rows,
        inverse_deviation,
    )


def layer_norm_backward(incoming_gradient, standardized_rows, inverse_deviation, norm_gain):
    scaled_rows = incoming_gradient * norm_gain.astype(jnp.float32)
    return inverse_deviation * (
        scaled_rows
        - jnp.mean(scaled_rows, axis=-1, keepdims=True)
        - standardized_rows * jnp.mean(scaled_rows * standardized_rows, axis=-1, keepdims=True)
    )


def contract_rows(left, right):
    return lax.dot_general(
        left, right, (((0,), (0,)), ((), ())), preferred_element_type=jnp.float32
    )


def against(left, right):
    return lax.dot_general(
        left, right, (((1,), (1,)), ((), ())), preferred_element_type=jnp.float32
    )


def exact_gelu(values):
    return jax.nn.gelu(values, approximate=False)


def image_forward(parts):
    query, keys, values = parts
    factor = float(query.shape[2]) ** (-0.5)
    scores = jnp.einsum("qhd,khd->hqk", query, keys, preferred_element_type=jnp.float32) * factor
    top = jnp.max(scores, axis=-1, keepdims=True)
    totals = jnp.sum(jnp.exp(scores - top), axis=-1, keepdims=True)
    logsum = top + jnp.log(totals)
    probs = jnp.exp(scores - logsum).astype(jnp.bfloat16)
    mixed = jnp.einsum("hqk,khd->qhd", probs, values, preferred_element_type=jnp.float32)
    return (mixed.astype(jnp.bfloat16), logsum)


def image_backward(parts):
    query, keys, values, logsum, grad_mixed = parts
    factor = float(query.shape[2]) ** (-0.5)
    scores = jnp.einsum("qhd,khd->hqk", query, keys, preferred_element_type=jnp.float32) * factor
    probs = jnp.exp(scores - logsum)
    grad_probs = jnp.einsum("qhd,khd->hqk", grad_mixed, values, preferred_element_type=jnp.float32)
    grad_scores = probs * (grad_probs - jnp.sum(probs * grad_probs, axis=-1, keepdims=True))
    rounded = grad_scores.astype(jnp.bfloat16)
    grad_query = (
        jnp.einsum("hqk,khd->qhd", rounded, keys, preferred_element_type=jnp.float32) * factor
    )
    grad_keys = (
        jnp.einsum("hqk,qhd->khd", rounded, query, preferred_element_type=jnp.float32) * factor
    )
    grad_values = jnp.einsum(
        "hqk,qhd->khd", probs.astype(jnp.bfloat16), grad_mixed, preferred_element_type=jnp.float32
    )
    return (
        grad_query.astype(jnp.bfloat16),
        grad_keys.astype(jnp.bfloat16),
        grad_values.astype(jnp.bfloat16),
    )


def squared_total(grads, tensor_count):
    total = jnp.zeros((), jnp.float32)
    for incoming_gradient, shared in zip(grads, shared_terms):
        weight = 1.0 / tensor_count if shared else 1.0
        total = total + weight * jnp.sum(incoming_gradient * incoming_gradient)
    return total


def adam_step(master, row_mean, square, incoming_gradient, rate):
    mean_new = 0.5 * row_mean + 0.5 * incoming_gradient
    square_new = 0.5 * square + 0.5 * incoming_gradient * incoming_gradient
    change = -rate * (mean_new / (jnp.sqrt(square_new) + 1e-08) + 0.1 * master)
    updated = master + change
    return [updated, mean_new, square_new, updated.astype(jnp.bfloat16)]


def per_device(
    images,
    valid_flags,
    cotangent,
    first_gain,
    first_shift,
    triple_weight,
    pair_bias,
    output_weight,
    output_bias,
    second_gain,
    second_shift,
    expand_weight,
    expand_bias,
    reduce_weight,
    reduce_bias,
    first_gain_mean,
    first_shift_mean,
    triple_weight_mean,
    pair_bias_mean,
    output_weight_mean,
    output_bias_mean,
    second_gain_mean,
    second_shift_mean,
    expand_weight_mean,
    expand_bias_mean,
    reduce_weight_mean,
    reduce_bias_mean,
    first_gain_square,
    first_shift_square,
    triple_weight_square,
    pair_bias_square,
    output_weight_square,
    output_bias_square,
    second_gain_square,
    second_shift_square,
    expand_weight_square,
    expand_bias_square,
    reduce_weight_square,
    reduce_bias_square,
):
    masters = (
        first_gain,
        first_shift,
        triple_weight,
        pair_bias,
        output_weight,
        output_bias,
        second_gain,
        second_shift,
        expand_weight,
        expand_bias,
        reduce_weight,
        reduce_bias,
    )
    means = (
        first_gain_mean,
        first_shift_mean,
        triple_weight_mean,
        pair_bias_mean,
        output_weight_mean,
        output_bias_mean,
        second_gain_mean,
        second_shift_mean,
        expand_weight_mean,
        expand_bias_mean,
        reduce_weight_mean,
        reduce_bias_mean,
    )
    squares = (
        first_gain_square,
        first_shift_square,
        triple_weight_square,
        pair_bias_square,
        output_weight_square,
        output_bias_square,
        second_gain_square,
        second_shift_square,
        expand_weight_square,
        expand_bias_square,
        reduce_weight_square,
        reduce_bias_square,
    )
    rounded = tuple((master.astype(jnp.bfloat16) for master in masters))
    (
        first_norm_gain,
        first_norm_bias,
        triple,
        pairs,
        out_weight,
        out_bias,
        second_norm_gain,
        second_norm_bias,
        up_weight,
        up_bias,
        down_weight,
        down_bias,
    ) = (
        lax.all_gather(rounded[0], "dp", axis=0, tiled=True),
        lax.all_gather(rounded[1], "dp", axis=0, tiled=True),
        lax.all_gather(rounded[2], "dp", axis=1, tiled=True),
        lax.all_gather(rounded[3], "dp", axis=2, tiled=True),
        lax.all_gather(rounded[4], "dp", axis=1, tiled=True),
        lax.all_gather(rounded[5], "dp", axis=0, tiled=True),
        lax.all_gather(rounded[6], "dp", axis=0, tiled=True),
        lax.all_gather(rounded[7], "dp", axis=0, tiled=True),
        lax.all_gather(rounded[8], "dp", axis=0, tiled=True),
        lax.all_gather(rounded[9], "dp", axis=1, tiled=True),
        lax.all_gather(rounded[10], "dp", axis=1, tiled=True),
        lax.all_gather(rounded[11], "dp", axis=0, tiled=True),
    )
    shape = images.shape
    count = shape[0] * shape[1]
    heads_local = pairs.shape[1]
    head_size = pairs.shape[2]
    split = (shape[0], shape[1], heads_local, head_size)
    tensor_count = lax.axis_size("tensor")
    input_row_block = images.reshape(count, shape[2]).astype(jnp.float32)
    first_normed_rows, first_standardized, first_inverse_deviation = apply_layer_norm(
        input_row_block, first_norm_gain, first_norm_bias
    )
    inputs_one = first_normed_rows.astype(jnp.bfloat16)
    projected = jnp.einsum("td,cde->cte", inputs_one, triple, preferred_element_type=jnp.float32)
    pair_flat = pairs.reshape(2, -1).astype(jnp.float32)
    query = (projected[0] + pair_flat[0]).astype(jnp.bfloat16).reshape(split)
    keys = projected[1].astype(jnp.bfloat16).reshape(split)
    values = (projected[2] + pair_flat[1]).astype(jnp.bfloat16).reshape(split)
    mixed, logsum = lax.map(image_forward, (query, keys, values))
    mixed_flat = mixed.reshape(count, -1)
    attn_part = jnp.dot(mixed_flat, out_weight, preferred_element_type=jnp.float32)
    middle_state = input_row_block + lax.psum(attn_part, "tensor") + out_bias.astype(jnp.float32)
    second_normed_rows, second_standardized, second_inverse_deviation = apply_layer_norm(
        middle_state, second_norm_gain, second_norm_bias
    )
    inputs_two = second_normed_rows.astype(jnp.bfloat16)
    hidden = jnp.dot(inputs_two, up_weight, preferred_element_type=jnp.float32) + up_bias.reshape(
        -1
    ).astype(jnp.float32)
    active_full, gelu_back = jax.vjp(exact_gelu, hidden)
    active = active_full.astype(jnp.bfloat16)
    mlp_part = jnp.dot(active, down_weight, preferred_element_type=jnp.float32)
    result = middle_state + lax.psum(mlp_part, "tensor") + down_bias.astype(jnp.float32)
    block_output = result.astype(jnp.bfloat16)
    output_gradient = (
        cotangent.astype(jnp.float32) * valid_flags.astype(jnp.float32)[:, None, None]
    ).reshape(count, -1)
    grad_low = output_gradient.astype(jnp.bfloat16)
    grad_down_bias = jnp.sum(output_gradient, axis=0)
    grad_down_weight = contract_rows(active, grad_low)
    grad_active = against(grad_low, down_weight)
    grad_hidden = gelu_back(grad_active)[0]
    grad_up_bias = jnp.sum(grad_hidden, axis=0).reshape(up_bias.shape)
    hidden_low = grad_hidden.astype(jnp.bfloat16)
    grad_up_weight = contract_rows(inputs_two, hidden_low)
    second_normed_gradient = lax.psum(against(hidden_low, up_weight), "tensor")
    second_gain_gradient = jnp.sum(second_normed_gradient * second_standardized, axis=0)
    grad_shift_two = jnp.sum(second_normed_gradient, axis=0)
    middle_gradient = output_gradient + layer_norm_backward(
        second_normed_gradient, second_standardized, second_inverse_deviation, second_norm_gain
    )
    grad_out_bias = jnp.sum(middle_gradient, axis=0)
    middle_low = middle_gradient.astype(jnp.bfloat16)
    grad_out_weight = contract_rows(mixed_flat, middle_low)
    grad_mixed = against(middle_low, out_weight).astype(jnp.bfloat16).reshape(split)
    grad_query, grad_keys, grad_values = lax.map(
        image_backward, (query, keys, values, logsum, grad_mixed)
    )
    stacked = jnp.stack(
        [
            grad_query.reshape(count, -1),
            grad_keys.reshape(count, -1),
            grad_values.reshape(count, -1),
        ]
    )
    grad_pairs = jnp.stack(
        [
            jnp.sum(stacked[0].astype(jnp.float32), axis=0),
            jnp.sum(stacked[2].astype(jnp.float32), axis=0),
        ]
    ).reshape(pairs.shape)
    grad_triple = jnp.einsum("td,cte->cde", inputs_one, stacked, preferred_element_type=jnp.float32)
    back_one = jnp.einsum("cte,cde->td", stacked, triple, preferred_element_type=jnp.float32)
    first_normed_gradient = lax.psum(back_one, "tensor")
    first_gain_gradient = jnp.sum(first_normed_gradient * first_standardized, axis=0)
    grad_shift_one = jnp.sum(first_normed_gradient, axis=0)
    row_gradient = middle_gradient + layer_norm_backward(
        first_normed_gradient, first_standardized, first_inverse_deviation, first_norm_gain
    )
    grads = (
        first_gain_gradient,
        grad_shift_one,
        grad_triple,
        grad_pairs,
        grad_out_weight,
        grad_out_bias,
        second_gain_gradient,
        grad_shift_two,
        grad_up_weight,
        grad_up_bias,
        grad_down_weight,
        grad_down_bias,
    )
    summed = lax.psum(
        (
            grads[0],
            grads[1],
            grads[2],
            grads[3],
            grads[4],
            grads[5],
            grads[6],
            grads[7],
            grads[8],
            grads[9],
            grads[10],
            grads[11],
        ),
        "dp",
    )
    total = lax.psum(squared_total(summed, tensor_count), "tensor")
    position = lax.axis_index("dp")
    owned = tuple(
        (
            lax.dynamic_slice_in_dim(
                incoming_gradient, position * master.shape[dim], master.shape[dim], dim
            )
            for incoming_gradient, master, dim in zip(summed, masters, shard_dims)
        )
    )
    norm_value = jnp.sqrt(total)
    limit = math.sqrt(4 * D * D + 2 * D * FF + 8 * D + FF)
    factor = jnp.minimum(1.0, limit / (norm_value + 1e-06))
    updates = []
    for master, row_mean, square, incoming_gradient, rate in zip(
        masters, means, squares, owned, rates
    ):
        updates.extend(adam_step(master, row_mean, square, incoming_gradient * factor, rate))
    return (block_output.reshape(shape), row_gradient.reshape(shape), norm_value, *updates)


HEAD = 64
ROWS = 640
BLOCK = 160
SUB = 32
LANES = 128
BF = jnp.bfloat16
F32 = jnp.float32
NEG = -1e30
MESH = pl.DeviceIdType.MESH


def flip(index, pattern, bits):
    out = index
    for bit in range(bits):
        if (pattern >> bit) & 1:
            step = 1 << bit
            out = out + (1 - 2 * lax.rem(lax.div(index, step), 2)) * step
    return out


def nt(left, right):
    return lax.dot_general(left, right, (((1,), (1,)), ((), ())), preferred_element_type=F32)


def nn(left, right):
    return jnp.dot(left, right, preferred_element_type=F32)


def tile(index, size):
    return pl.ds(pl.multiple_of(index * size, size), size)


def rows32(start, size):
    return pl.ds(pl.multiple_of(start, SUB), size)


def center_scale(v):
    c = v - jnp.mean(v, axis=-1, keepdims=True)
    r = lax.rsqrt(jnp.mean(c * c, axis=-1, keepdims=True) + 1e-06)
    return c * r, r


SCRATCH = dict(
    xs=((ROWS, D), BF),
    gyb=((ROWS, D), BF),
    small_own=((8, LANES), F32),
    vec=((8, D), F32),
    vecb=((8, D), F32),
    bias3=((3, 1, 256), F32),
    ebias=((1, D), F32),
    wqkv=((3, D, 256), BF),
    wof=((D, D), BF),
    wr=((D, D), BF),
    we=((D, D), BF),
    a1=((ROWS, D), BF),
    a1t=((D, ROWS), BF),
    tt=((D, ROWS), BF),
    qkv=((3, ROWS, 256), BF),
    kt=((256, ROWS), BF),
    vt=((256, ROWS), BF),
    ot=((256, ROWS), BF),
    of=((ROWS, D), BF),
    lse=((4, 1, ROWS), F32),
    x1=((ROWS, D), F32),
    a2=((ROWS, D), BF),
    du=((ROWS, D), F32),
    hb=((ROWS, 256), F32),
    u=((ROWS, D), BF),
    dhb=((ROWS, D), BF),
    r3s=((3, BLOCK, D), BF),
    r3r=((3, BLOCK, D), BF),
    r2s=((3, BLOCK, D), BF),
    r2r=((3, BLOCK, D), BF),
    r4s=((3, BLOCK, D), BF),
    r4r=((3, BLOCK, D), BF),
    dxf=((ROWS, D), BF),
    dobs=((3, BLOCK, 256), BF),
    dob=((ROWS, 256), BF),
    ds4=((ROWS, 512), BF),
    p4=((ROWS, 512), BF),
    qm4=((512, 256), BF),
    dm4=((512, 256), BF),
    dk=((ROWS, 256), F32),
    dv=((ROWS, 256), F32),
    dqt=((256, LANES), F32),
    dqkv=((3, ROWS, 256), BF),
    yb=((ROWS, D), BF),
    xg=((ROWS, D), BF),
    gwr=((D, D), BF),
    gwe=((D, D), BF),
    gwo=((256, D), BF),
    gwq=((3, D, 256), BF),
    pr_r=((4, D, LANES), BF),
    pr_e=((4, LANES, D), BF),
    pr_o=((4, 256, LANES), BF),
    pr_q=((4, 3, LANES, 256), BF),
    cr_r=((3, D, LANES), BF),
    cr_e=((3, LANES, D), BF),
    cr_o=((3, 256, LANES), BF),
    cr_q=((3, 3, LANES, 256), BF),
    sg=((8, D), F32),
    sgz=((3, 8, D), F32),
    sgt=((8, D), F32),
    sgd=((7, 8, D), F32),
    nrm=((2, 8, LANES), F32),
    nrz=((3, 8, LANES), F32),
    nrd=((7, 8, LANES), F32),
)
SEMS = dict(
    ld=(8,),
    g_s=(5, 8),
    g_r=(5, 8),
    wz_s=(3,),
    wz_r=(3,),
    o_s=(5, 3),
    o_r=(5, 3),
    z_s=(9, 3),
    z_r=(9, 3),
    p_s=(4, 4),
    p_r=(4, 4),
    c_s=(4, 3),
    c_r=(4, 3),
    d_s=(2, 7),
    d_r=(2, 7),
)
INPUTS = dict(x_in=0, gy_in=0, small_in=0, q_in=0, o_in=0, e_in=0, r_in=0)
OUTPUTS = dict(gq=0, go=0, ge=0, gr=0, sg_out=0, total=0, y_out=0, xg_out=0)


def block_kernel(tokens, *refs):
    names = (*INPUTS, *OUTPUTS, *SCRATCH, *SEMS)
    R = types.SimpleNamespace(**dict(zip(names, refs)))
    me = lax.axis_index("dp")
    z = lax.axis_index("tensor")
    dpx = [flip(me, e, 3) for e in range(8)]
    zx = [flip(z, d, 2) for d in range(4)]
    sent = []

    def remote(src, dst, send, recv, where):
        return pltpu.make_async_remote_copy(
            src_ref=src, dst_ref=dst, send_sem=send, recv_sem=recv,
            device_id=where, device_id_type=MESH,
        )

    def post(copy):
        copy.start()
        sent.append(copy)

    barrier = pltpu.get_barrier_semaphore()
    for e in range(1, 8):
        pl.semaphore_signal(barrier, inc=1, device_id={"dp": dpx[e]}, device_id_type=MESH)
    for d in range(1, 4):
        pl.semaphore_signal(barrier, inc=1, device_id={"tensor": zx[d]}, device_id_type=MESH)
    loads = [
        pltpu.make_async_copy(a, b, R.ld.at[i])
        for i, (a, b) in enumerate(
            (
                (R.small_in, R.small_own),
                (R.q_in, R.gq),
                (R.o_in, R.go),
                (R.r_in, R.gr),
                (R.e_in, R.ge),
                (R.x_in, R.xs),
                (R.gy_in, R.gyb),
            )
        )
    ]
    for copy in loads:
        copy.start()

    GATHER = {
        "small": (0, lambda j: R.vec.at[:, tile(j, LANES)]),
        "q": (1, lambda j: R.wqkv.at[:, tile(j, LANES), :]),
        "o": (2, lambda j: R.wof.at[:, tile(j, LANES)]),
        "r": (3, lambda j: R.wr.at[:, tile(j, LANES)]),
        "e": (4, lambda j: R.we.at[tile(j, LANES), :]),
    }

    def gather_copy(name, source, target, slot):
        a, region = GATHER[name]
        part = region(dpx[source])
        return remote(part, part, R.g_s.at[a, slot], R.g_r.at[a, slot], {"dp": dpx[target]})

    def gather_send(name):
        for e in (6, 2, 4, 1):
            post(gather_copy(name, 0, e, e))

    def gather_pass(name):
        for e in (2, 4, 6):
            gather_copy(name, e, e, e).wait_recv()
            post(gather_copy(name, e, 1, e + 1))

    def gather_wait(name):
        for e in (1, 3, 5, 7):
            gather_copy(name, e, 1, e).wait_recv()

    own = tile(me, LANES)
    loads[0].wait()
    R.vec[:, own] = R.small_own[...]
    loads[1].wait()
    R.wqkv[:, own, :] = R.gq[...].astype(BF)
    loads[2].wait()
    R.wof[tile(z, 256), own] = R.go[...].astype(BF)
    pl.semaphore_wait(barrier, 10)
    gather_send("small")
    gather_send("q")
    for d in (3, 2, 1):
        part = R.wof.at[tile(z, 256), own]
        post(remote(part, part, R.wz_s.at[d - 1], R.wz_r.at[d - 1], {"tensor": zx[d]}))
    loads[3].wait()
    R.wr[:, own] = R.gr[...].astype(BF)
    loads[4].wait()
    R.we[own, :] = R.ge[...].astype(BF)
    for d in (1, 2, 3):
        part = R.wof.at[tile(zx[d], 256), own]
        remote(part, part, R.wz_s.at[d - 1], R.wz_r.at[d - 1], {"tensor": zx[d]}).wait_recv()
    gather_send("o")
    gather_send("r")
    gather_send("e")

    gather_pass("small")
    gather_wait("small")
    R.vecb[...] = R.vec[...].astype(BF).astype(F32)
    spread_row = lax.broadcasted_iota(jnp.int32, (LANES, D), 0)
    spread_col = lax.broadcasted_iota(jnp.int32, (LANES, D), 1)
    spread = jnp.where(
        (lax.div(spread_row, 8) == lax.div(spread_col, 64))
        & (lax.rem(spread_row, 8) == lax.rem(spread_col, 8)),
        1.0,
        0.0,
    ).astype(BF)
    turn = lax.rem(lax.div(lax.broadcasted_iota(jnp.int32, (8, D), 1), 8), 8)
    pick = turn == lax.broadcasted_iota(jnp.int32, (8, D), 0)

    def unpack(row):
        parts = jnp.concatenate(
            [R.vecb[row : row + 1, j * LANES : (j + 1) * LANES] for j in range(8)], axis=0
        ).astype(BF)
        wide = nn(parts, spread)
        return jnp.sum(jnp.where(pick, wide, 0.0), axis=0, keepdims=True)

    R.ebias[...] = unpack(6)
    pair = unpack(7)
    R.bias3[0] = pair[:, :256]
    R.bias3[1] = jnp.zeros((1, 256), F32)
    R.bias3[2] = pair[:, 256:512]

    loads[5].wait()
    gain1, shift1 = R.vecb[0:1, :], R.vecb[1:2, :]
    sub_iota = lax.broadcasted_iota(jnp.int32, (SUB, 1), 0)

    @pl.loop(0, ROWS // SUB)
    def _(b):
        rows = tile(b, SUB)
        hat, _ = center_scale(R.xs[rows, :].astype(F32))
        out = jnp.where(sub_iota + b * SUB < tokens, hat * gain1 + shift1, 0.0)
        R.a1[rows, :] = out.astype(BF)

    def flip_into(target, source):
        @pl.loop(0, D // LANES)
        def _(i):
            target[tile(i, LANES), :] = source[:, tile(i, LANES)].T

    flip_into(R.a1t, R.a1)

    gather_pass("q")
    gather_wait("q")

    @pl.loop(0, 3)
    def _(c):
        acc = nn(R.a1[...], R.wqkv[c]) + R.bias3[c]
        R.qkv[c] = acc.astype(BF)

    scale = jnp.asarray(HEAD ** (-0.5), BF)
    R.qkv[0] = R.qkv[0] * scale
    R.kt[...] = R.qkv[1].T
    R.vt[...] = R.qkv[2].T
    head_lane = lax.div(lax.broadcasted_iota(jnp.int32, (LANES, 256), 1), HEAD)
    edge = tokens // 64 * 64
    tail_iota = lax.broadcasted_iota(jnp.int32, (ROWS - edge, LANES), 0) + edge

    def masked_scores(query):
        s = nt(R.qkv[1], query)
        return jnp.concatenate([s[:edge], jnp.where(tail_iota < tokens, s[edge:], NEG)], axis=0)

    def only_head(value, h):
        return jnp.where(head_lane == h, value, jnp.zeros_like(value))

    def o_copy(b, d, source):
        part = R.of.at[tile(b, LANES), tile(zx[source], 256)]
        return remote(part, part, R.o_s.at[b, d - 1], R.o_r.at[b, d - 1], {"tensor": zx[d]})

    @pl.loop(0, ROWS // LANES)
    def _(b):
        cols = tile(b, LANES)
        query = R.qkv[0, cols, :]
        for h in range(4):
            s = masked_scores(only_head(query, h))
            top = jnp.max(s, axis=0, keepdims=True)
            p = jnp.exp(s - top)
            total = jnp.sum(p, axis=0, keepdims=True)
            R.lse[h, :, cols] = top + jnp.log(total)
            pb = (p * (1.0 / total)).astype(BF)
            mixed = nn(R.vt[h * HEAD : (h + 1) * HEAD, :], pb)
            R.ot[h * HEAD : (h + 1) * HEAD, cols] = mixed.astype(BF)
        R.of[cols, tile(z, 256)] = R.ot[:, cols].T
        for d in (3, 2, 1):
            o_copy(b, d, 0).start()

    gather_pass("o")
    loads[6].wait()
    gather_pass("r")
    gather_wait("r")

    @pl.loop(0, 4)
    def _(n):
        R.du[:, tile(n, 256)] = nt(R.gyb[...], R.wr[tile(n, 256), :])

    gather_wait("o")
    out_bias = R.vecb[2:3, :]
    gain2, shift2 = R.vecb[3:4, :], R.vecb[4:5, :]

    @pl.loop(0, ROWS // LANES)
    def _(b):
        rows = tile(b, LANES)
        for d in (1, 2, 3):
            o_copy(b, d, d).wait_recv()

        @pl.loop(0, 4)
        def _(n):
            cols = tile(n, 256)
            R.x1[rows, cols] = R.xs[rows, cols].astype(F32) + nn(R.of[rows, :], R.wof[:, cols])

        @pl.loop(0, LANES // SUB)
        def _(i):
            part = rows32(b * LANES + i * SUB, SUB)
            v = R.x1[part, :] + out_bias
            R.x1[part, :] = v
            hat, _ = center_scale(v)
            R.a2[part, :] = (hat * gain2 + shift2).astype(BF)

    gather_pass("e")
    gather_wait("e")

    @pl.loop(0, 4)
    def _(n):
        cols = tile(n, 256)
        R.hb[...] = nn(R.a2[...], R.we[:, cols]) + R.ebias[:, cols]

        def part(i, total):
            rows = tile(i, SUB)
            h = R.hb[rows, :]
            cdf = 0.5 * (1.0 + lax.erf(h * math.sqrt(0.5)))
            slope = cdf + h * (jnp.exp(-0.5 * h * h) * (1.0 / math.sqrt(2.0 * math.pi)))
            dh = R.du[rows, cols] * slope
            R.u[rows, cols] = (h * cdf).astype(BF)
            R.dhb[rows, cols] = dh.astype(BF)
            return total + jnp.sum(dh, axis=0, keepdims=True)

        R.sg[6:7, cols] = lax.fori_loop(0, ROWS // SUB, part, jnp.zeros((1, 256), F32))

    def z_copy(x, d, src, dst):
        return remote(src, dst, R.z_s.at[x, d - 1], R.z_r.at[x, d - 1], {"tensor": zx[d]})

    def z_scatter(x, d, s, r):
        return z_copy(x, d, s.at[d - 1], r.at[d - 1])

    for d in (3, 2, 1, 0):
        rows = rows32(zx[d] * BLOCK, BLOCK)

        @pl.loop(0, 4)
        def _(n):
            cols = tile(n, 256)
            part = nt(R.dhb[rows, :], R.we[cols, :])
            if d:
                R.r3s[d - 1, :, cols] = part.astype(BF)
            else:
                R.du[0:BLOCK, cols] = part

        if d:
            post(z_scatter(0, d, R.r3s, R.r3r))

    PIECES = {
        "r": (0, R.pr_r, R.cr_r, R.gr, lambda j: R.gwr.at[:, tile(j, LANES)]),
        "e": (1, R.pr_e, R.cr_e, R.ge, lambda j: R.gwe.at[tile(j, LANES), :]),
        "o": (2, R.pr_o, R.cr_o, R.go, lambda j: R.gwo.at[:, tile(j, LANES)]),
        "q": (3, R.pr_q, R.cr_q, R.gq, lambda j: R.gwq.at[:, tile(j, LANES), :]),
    }

    def pair_copy(name, t):
        a, pr, _, _, piece = PIECES[name]
        return remote(
            piece(dpx[2 * t + 1]), pr.at[t], R.p_s.at[a, t], R.p_r.at[a, t], {"dp": dpx[1]}
        )

    def cross_copy(name, t):
        a, _, cr, _, piece = PIECES[name]
        return remote(
            piece(dpx[2 * t]), cr.at[t - 1], R.c_s.at[a, t - 1], R.c_r.at[a, t - 1],
            {"dp": dpx[2 * t]},
        )

    def pair_send(name):
        for t in (3, 1, 2, 0):
            post(pair_copy(name, t))

    def pair_sum(name):
        _, pr, _, out, piece = PIECES[name]
        for t in (3, 1, 2, 0):
            pair_copy(name, t).wait_recv()
            held = piece(dpx[2 * t])
            both = held[...].astype(F32) + pr[t].astype(F32)
            if t:
                held[...] = both.astype(BF)
                post(cross_copy(name, t))
            else:
                out[...] = both

    def cross_sum(name):
        _, _, cr, out, _ = PIECES[name]
        for t in (1, 2, 3):
            cross_copy(name, t).wait_recv()
        both = out[...] + cr[0].astype(F32) + cr[1].astype(F32) + cr[2].astype(F32)
        out[...] = both
        return jnp.sum(both * both)

    flip_into(R.tt, R.u)

    @pl.loop(0, 4)
    def _(n):
        R.gwr[:, tile(n, 256)] = nn(R.tt[...], R.gyb[:, tile(n, 256)]).astype(BF)

    pair_send("r")
    flip_into(R.tt, R.a2)

    @pl.loop(0, 4)
    def _(n):
        R.gwe[:, tile(n, 256)] = nn(R.tt[...], R.dhb[:, tile(n, 256)]).astype(BF)

    pair_send("e")
    pair_sum("r")

    for d in (3, 2, 1, 0):
        rows = rows32(zx[d] * BLOCK, BLOCK)

        @pl.loop(0, 4)
        def _(n):
            cols = tile(n, 256)
            part = nn(R.u[rows, :], R.wr[:, cols])
            if d:
                R.r2s[d - 1, :, cols] = part.astype(BF)
            else:
                R.du[BLOCK : 2 * BLOCK, cols] = part

    pair_sum("e")

    mine = z * BLOCK
    mine_rows = rows32(mine, BLOCK)
    for d in (1, 2, 3):
        z_scatter(0, d, R.r3s, R.r3r).wait_recv()

    def norm_part(i, sums):
        local = tile(i, SUB)
        rows = rows32(mine + i * SUB, SUB)
        dxn = (
            R.du[local, :]
            + R.r3r[0, local, :].astype(F32)
            + R.r3r[1, local, :].astype(F32)
            + R.r3r[2, local, :].astype(F32)
        )
        hat, r = center_scale(R.x1[rows, :])
        gy = R.gyb[rows, :].astype(F32)
        e = dxn * gain2
        dx = gy + r * (
            e
            - jnp.mean(e, axis=-1, keepdims=True)
            - hat * jnp.mean(e * hat, axis=-1, keepdims=True)
        )
        R.du[rows32(3 * BLOCK + i * SUB, SUB), :] = dx
        R.dxf[rows, :] = dx.astype(BF)
        terms = (dxn * hat, dxn, dx, gy)
        return tuple(s + jnp.sum(t, axis=0, keepdims=True) for s, t in zip(sums, terms))

    nothing = jnp.zeros((1, D), F32)
    sums = lax.fori_loop(0, BLOCK // SUB, norm_part, (nothing,) * 4)
    R.sg[3:4, :] = sums[0]
    R.sg[4:5, :] = sums[1]
    R.sg[2:3, :] = sums[2]
    R.sg[5:6, :] = sums[3]

    def dob_copy(d):
        return z_copy(1, d, R.dobs.at[d - 1], R.dob.at[mine_rows, :])

    for d in (3, 2, 1, 0):
        part = nt(R.dxf[mine_rows, :], R.wof[tile(zx[d], 256), :]).astype(BF)
        if d:
            R.dobs[d - 1] = part
            post(dob_copy(d))
        else:
            R.dob[mine_rows, :] = part

    def z_spread(x, d, ref, source):
        part = ref.at[rows32(zx[source] * BLOCK, BLOCK), :]
        return z_copy(x, d, part, part)

    for d in (3, 2, 1):
        post(z_spread(2, d, R.dxf, 0))
    for d in (3, 2, 1):
        post(z_scatter(3, d, R.r2s, R.r2r))

    for d in (1, 2, 3):
        z_copy(1, d, R.dobs.at[d - 1], R.dob.at[rows32(zx[d] * BLOCK, BLOCK), :]).wait_recv()
    R.dk[...] = jnp.zeros_like(R.dk)
    R.dv[...] = jnp.zeros_like(R.dv)
    down_bias = R.vecb[5:6, :]

    @pl.loop(0, ROWS // LANES)
    def _(b):
        cols = tile(b, LANES)
        query = R.qkv[0, cols, :]
        grad = R.dob[cols, :]
        for h in range(4):
            lanes = slice(h * LANES, (h + 1) * LANES)
            qm = only_head(query, h)
            dm = only_head(grad, h)
            R.qm4[lanes, :] = qm
            R.dm4[lanes, :] = dm
            p = jnp.exp(masked_scores(qm) - R.lse[h, :, cols])
            R.p4[:, lanes] = p.astype(BF)
            dp = nt(R.qkv[2], dm)
            ds = (p * (dp - jnp.sum(p * dp, axis=0, keepdims=True))).astype(BF)
            R.ds4[:, lanes] = ds
            R.dqt[h * HEAD : (h + 1) * HEAD, :] = nn(R.kt[h * HEAD : (h + 1) * HEAD, :], ds)
        R.dqkv[0, cols, :] = (R.dqt[...].T * HEAD ** (-0.5)).astype(BF)
        R.dk[...] += nn(R.ds4[...], R.qm4[...])
        R.dv[...] += nn(R.p4[...], R.dm4[...])

    R.dqkv[1] = R.dk[...].astype(BF)
    R.dqkv[2] = R.dv[...].astype(BF)

    for d in (1, 2, 3):
        z_scatter(3, d, R.r2s, R.r2r).wait_recv()

    @pl.loop(0, BLOCK // SUB)
    def _(i):
        local = tile(i, SUB)
        rows = rows32(mine + i * SUB, SUB)
        y = (
            R.x1[rows, :]
            + R.du[rows32(BLOCK + i * SUB, SUB), :]
            + R.r2r[0, local, :].astype(F32)
            + R.r2r[1, local, :].astype(F32)
            + R.r2r[2, local, :].astype(F32)
            + down_bias
        )
        R.yb[rows, :] = y.astype(BF)

    for c in range(3):
        R.gwq[c] = nn(R.a1t[...], R.dqkv[c]).astype(BF)
    pair_send("q")
    R.sg[7:8, :] = jnp.concatenate(
        [
            jnp.sum(R.dqkv[0].astype(F32), axis=0, keepdims=True),
            jnp.sum(R.dqkv[2].astype(F32), axis=0, keepdims=True),
            jnp.zeros((1, 512), F32),
        ],
        axis=1,
    )
    R.sg[0:2, :] = jnp.zeros((2, D), F32)
    for d in (3, 2, 1, 0):
        start = zx[d] * BLOCK
        rows = rows32(start, BLOCK)

        @pl.loop(0, 4)
        def _(n):
            cols = tile(n, 256)
            R.du[0:BLOCK, cols] = (
                nt(R.dqkv[0, rows, :], R.wqkv[0, cols, :])
                + nt(R.dqkv[1, rows, :], R.wqkv[1, cols, :])
                + nt(R.dqkv[2, rows, :], R.wqkv[2, cols, :])
            )

        def first_part(i, sums):
            local = tile(i, SUB)
            dxn = R.du[local, :]
            hat, _ = center_scale(R.xs[rows32(start + i * SUB, SUB), :].astype(F32))
            if d:
                R.r4s[d - 1, local, :] = dxn.astype(BF)
            terms = (dxn * hat, dxn)
            return tuple(s + jnp.sum(t, axis=0, keepdims=True) for s, t in zip(sums, terms))

        sums = lax.fori_loop(0, BLOCK // SUB, first_part, (nothing,) * 2)
        R.sg[0:1, :] += sums[0]
        R.sg[1:2, :] += sums[1]

    for d in (3, 2, 1):
        post(z_copy(7, d, R.sg, R.sgz.at[d - 1]))
    for d in (3, 2, 1):
        post(z_scatter(5, d, R.r4s, R.r4r))
    for d in (3, 2, 1):
        post(z_spread(4, d, R.yb, 0))
    pair_sum("q")
    for d in (1, 2, 3):
        z_spread(2, d, R.dxf, d).wait_recv()
    R.gwo[...] = nn(R.ot[...], R.dxf[...]).astype(BF)
    pair_send("o")
    squares = cross_sum("r")
    squares += cross_sum("e")
    pair_sum("o")

    for d in (1, 2, 3):
        z_copy(7, d, R.sg, R.sgz.at[d - 1]).wait_recv()
    shared_row = lax.broadcasted_iota(jnp.int32, (8, D), 0) < 6
    others = R.sgz[0] + R.sgz[1] + R.sgz[2]
    R.sgt[...] = R.sg[...] + jnp.where(shared_row, others, 0.0)

    def d_copy(x, e, src, dst):
        return remote(src, dst, R.d_s.at[x, e - 1], R.d_r.at[x, e - 1], {"dp": dpx[e]})

    for e in (6, 7, 2, 3, 4, 5, 1):
        post(d_copy(0, e, R.sgt, R.sgd.at[e - 1]))

    for d in (1, 2, 3):
        z_scatter(5, d, R.r4s, R.r4r).wait_recv()

    @pl.loop(0, BLOCK // SUB)
    def _(i):
        local = tile(i, SUB)
        rows = rows32(mine + i * SUB, SUB)
        dxn = (
            R.du[local, :]
            + R.r4r[0, local, :].astype(F32)
            + R.r4r[1, local, :].astype(F32)
            + R.r4r[2, local, :].astype(F32)
        )
        hat, r = center_scale(R.xs[rows, :].astype(F32))
        e = dxn * gain1
        dx = R.du[rows32(3 * BLOCK + i * SUB, SUB), :] + r * (
            e
            - jnp.mean(e, axis=-1, keepdims=True)
            - hat * jnp.mean(e * hat, axis=-1, keepdims=True)
        )
        R.xg[rows, :] = dx.astype(BF)

    for d in (3, 2, 1):
        post(z_spread(6, d, R.xg, 0))

    squares += cross_sum("q")
    squares += cross_sum("o")
    for e in range(1, 8):
        d_copy(0, e, R.sgt, R.sgd.at[e - 1]).wait_recv()
    sg = R.sgt[...]
    for e in range(1, 8):
        sg = sg + R.sgd[e - 1]
    R.sg_out[...] = sg
    squared = sg * sg
    shared_squares = jnp.sum(jnp.where(shared_row, squared, 0.0))
    local_squares = jnp.sum(jnp.where(shared_row, 0.0, squared))
    R.nrm[0] = jnp.full((8, LANES), squares + local_squares * 0.125, F32)
    for e in (6, 7, 2, 3, 4, 5, 1):
        post(d_copy(1, e, R.nrm.at[0], R.nrd.at[e - 1]))
    for e in range(1, 8):
        d_copy(1, e, R.nrm.at[0], R.nrd.at[e - 1]).wait_recv()
    value = R.nrm[0]
    for e in range(1, 8):
        value = value + R.nrd[e - 1]
    R.nrm[1] = value
    for d in (3, 2, 1):
        post(z_copy(8, d, R.nrm.at[1], R.nrz.at[d - 1]))

    for d in (1, 2, 3):
        z_spread(4, d, R.yb, d).wait_recv()
    y_store = pltpu.make_async_copy(R.yb, R.y_out, R.ld.at[0])
    y_store.start()
    for d in (1, 2, 3):
        z_spread(6, d, R.xg, d).wait_recv()
    x_store = pltpu.make_async_copy(R.xg, R.xg_out, R.ld.at[1])
    x_store.start()
    for d in (1, 2, 3):
        z_copy(8, d, R.nrm.at[1], R.nrz.at[d - 1]).wait_recv()
    R.total[...] = R.nrm[1] + R.nrz[0] + R.nrz[1] + R.nrz[2] + shared_squares
    for copy in sent:
        copy.wait_send()

    @pl.loop(0, ROWS // LANES)
    def _(b):
        for d in (1, 2, 3):
            o_copy(b, d, 0).wait_send()

    y_store.wait()
    x_store.wait()


def run_block(tokens, x_rows, gy_rows, small, triple, out, up, down):
    kernel = functools.partial(block_kernel, tokens)
    vmem = pl.BlockSpec(memory_space=pltpu.VMEM)
    anywhere = pl.BlockSpec(memory_space=pl.ANY)
    return pl.pallas_call(
        kernel,
        out_shape=(
            jax.ShapeDtypeStruct((3, LANES, 256), F32),
            jax.ShapeDtypeStruct((256, LANES), F32),
            jax.ShapeDtypeStruct((LANES, D), F32),
            jax.ShapeDtypeStruct((D, LANES), F32),
            jax.ShapeDtypeStruct((8, D), F32),
            jax.ShapeDtypeStruct((8, LANES), F32),
            jax.ShapeDtypeStruct((ROWS, D), BF),
            jax.ShapeDtypeStruct((ROWS, D), BF),
        ),
        in_specs=[anywhere] * len(INPUTS),
        out_specs=(vmem,) * 6 + (anywhere,) * 2,
        scratch_shapes=[
            *(pltpu.VMEM(shape, dtype) for shape, dtype in SCRATCH.values()),
            *(pltpu.SemaphoreType.DMA(shape) for shape in SEMS.values()),
        ],
        compiler_params=pltpu.CompilerParams(
            collective_id=0, has_side_effects=True, vmem_limit_bytes=63 * 1024 * 1024
        ),
        name="block_step",
    )(x_rows, gy_rows, small, triple, out, up, down)


def fused_device(*args):
    images, valid_flags, cotangent = args[:3]
    masters, means, squares = args[3:15], args[15:27], args[27:39]
    tokens = images.shape[1]
    pad = ((0, ROWS - tokens), (0, 0))
    x_rows = jnp.pad(images[0], pad)
    gy_rows = jnp.pad(cotangent[0] * valid_flags[0].astype(BF), pad)
    vectors = [masters[i].reshape(1, LANES) for i in (0, 1, 5, 6, 7, 11)]
    small = jnp.concatenate(
        [
            *vectors,
            masters[9].reshape(1, LANES),
            jnp.pad(masters[3].reshape(1, HEAD), ((0, 0), (0, LANES - HEAD))),
        ],
        axis=0,
    )
    gq, go, ge, gr, sg, total, y_rows, grad_rows = run_block(
        tokens, x_rows, gy_rows, small, masters[2], masters[4], masters[8], masters[10]
    )
    position = lax.axis_index("dp")
    owned = lax.dynamic_slice_in_dim(sg[:6], position * LANES, LANES, 1)
    expand = lax.dynamic_slice_in_dim(sg[6].reshape(16, 64), position * 8, 8, 1)
    pairs = lax.dynamic_slice_in_dim(sg[7, :512].reshape(2, 4, 64), position * 8, 8, 2)
    grads = (
        owned[0], owned[1], gq, pairs, go, owned[2], owned[3], owned[4], ge, expand, gr, owned[5],
    )
    norm_value = jnp.sqrt(total[0, 0])
    limit = math.sqrt(4 * D * D + 2 * D * FF + 8 * D + FF)
    factor = jnp.minimum(1.0, limit / (norm_value + 1e-06))
    updates = []
    for master, row_mean, square, gradient, rate in zip(masters, means, squares, grads, rates):
        updates.extend(adam_step(master, row_mean, square, gradient * factor, rate))
    return (
        y_rows[:tokens].reshape(images.shape),
        grad_rows[:tokens].astype(F32).reshape(images.shape),
        norm_value,
        *updates,
    )


def solution(mesh):
    in_specs = (
        P("dp", None, None),
        P("dp"),
        P("dp", None, None),
        P("dp"),
        P("dp"),
        P(None, "dp", "tensor"),
        P(None, "tensor", "dp"),
        P("tensor", "dp"),
        P("dp"),
        P("dp"),
        P("dp"),
        P("dp", "tensor"),
        P("tensor", "dp"),
        P("tensor", "dp"),
        P("dp"),
        P("dp"),
        P("dp"),
        P(None, "dp", "tensor"),
        P(None, "tensor", "dp"),
        P("tensor", "dp"),
        P("dp"),
        P("dp"),
        P("dp"),
        P("dp", "tensor"),
        P("tensor", "dp"),
        P("tensor", "dp"),
        P("dp"),
        P("dp"),
        P("dp"),
        P(None, "dp", "tensor"),
        P(None, "tensor", "dp"),
        P("tensor", "dp"),
        P("dp"),
        P("dp"),
        P("dp"),
        P("dp", "tensor"),
        P("tensor", "dp"),
        P("tensor", "dp"),
        P("dp"),
    )
    out_specs = (
        P("dp", None, None),
        P("dp", None, None),
        P(),
        P("dp"),
        P("dp"),
        P("dp"),
        P("dp"),
        P("dp"),
        P("dp"),
        P("dp"),
        P("dp"),
        P(None, "dp", "tensor"),
        P(None, "dp", "tensor"),
        P(None, "dp", "tensor"),
        P(None, "dp", "tensor"),
        P(None, "tensor", "dp"),
        P(None, "tensor", "dp"),
        P(None, "tensor", "dp"),
        P(None, "tensor", "dp"),
        P("tensor", "dp"),
        P("tensor", "dp"),
        P("tensor", "dp"),
        P("tensor", "dp"),
        P("dp"),
        P("dp"),
        P("dp"),
        P("dp"),
        P("dp"),
        P("dp"),
        P("dp"),
        P("dp"),
        P("dp"),
        P("dp"),
        P("dp"),
        P("dp"),
        P("dp", "tensor"),
        P("dp", "tensor"),
        P("dp", "tensor"),
        P("dp", "tensor"),
        P("tensor", "dp"),
        P("tensor", "dp"),
        P("tensor", "dp"),
        P("tensor", "dp"),
        P("tensor", "dp"),
        P("tensor", "dp"),
        P("tensor", "dp"),
        P("tensor", "dp"),
        P("dp"),
        P("dp"),
        P("dp"),
        P("dp"),
    )
    fused = mesh.shape["dp"] == 8 and mesh.shape["tensor"] == 4
    return jax.shard_map(
        fused_device if fused else per_device, mesh=mesh, in_specs=in_specs, out_specs=out_specs, check_vma=False
    )
```

```python
import functools
import math
import types

import jax
import jax.numpy as jnp
from jax import lax
from jax.experimental import pallas as pl
from jax.experimental.pallas import tpu as pltpu
from jax.sharding import PartitionSpec as P

D = 1024
FF = 4096


shard_dims = (0, 0, 1, 2, 1, 0, 0, 0, 0, 1, 1, 0)
shared_terms = (1, 1, 0, 0, 0, 1, 1, 1, 0, 0, 0, 1)
rates = (0.2, 0.2, 0.03, 0.2, 0.03, 0.2, 0.2, 0.2, 0.03, 0.2, 0.03, 0.2)


def apply_layer_norm(input_row_block, norm_gain, norm_bias):
    center = jnp.mean(input_row_block, axis=-1, keepdims=True)
    centered_rows = input_row_block - center
    inverse_deviation = lax.rsqrt(
        jnp.mean(centered_rows * centered_rows, axis=-1, keepdims=True) + 1e-06
    )
    standardized_rows = centered_rows * inverse_deviation
    return (
        standardized_rows * norm_gain.astype(jnp.float32) + norm_bias.astype(jnp.float32),
        standardized_rows,
        inverse_deviation,
    )


def layer_norm_backward(incoming_gradient, standardized_rows, inverse_deviation, norm_gain):
    scaled_rows = incoming_gradient * norm_gain.astype(jnp.float32)
    return inverse_deviation * (
        scaled_rows
        - jnp.mean(scaled_rows, axis=-1, keepdims=True)
        - standardized_rows * jnp.mean(scaled_rows * standardized_rows, axis=-1, keepdims=True)
    )


def contract_rows(left, right):
    return lax.dot_general(
        left, right, (((0,), (0,)), ((), ())), preferred_element_type=jnp.float32
    )


def against(left, right):
    return lax.dot_general(
        left, right, (((1,), (1,)), ((), ())), preferred_element_type=jnp.float32
    )


def exact_gelu(values):
    return jax.nn.gelu(values, approximate=False)


def image_forward(parts):
    query, keys, values = parts
    factor = float(query.shape[2]) ** (-0.5)
    scores = jnp.einsum("qhd,khd->hqk", query, keys, preferred_element_type=jnp.float32) * factor
    top = jnp.max(scores, axis=-1, keepdims=True)
    totals = jnp.sum(jnp.exp(scores - top), axis=-1, keepdims=True)
    logsum = top + jnp.log(totals)
    probs = jnp.exp(scores - logsum).astype(jnp.bfloat16)
    mixed = jnp.einsum("hqk,khd->qhd", probs, values, preferred_element_type=jnp.float32)
    return (mixed.astype(jnp.bfloat16), logsum)


def image_backward(parts):
    query, keys, values, logsum, grad_mixed = parts
    factor = float(query.shape[2]) ** (-0.5)
    scores = jnp.einsum("qhd,khd->hqk", query, keys, preferred_element_type=jnp.float32) * factor
    probs = jnp.exp(scores - logsum)
    grad_probs = jnp.einsum("qhd,khd->hqk", grad_mixed, values, preferred_element_type=jnp.float32)
    grad_scores = probs * (grad_probs - jnp.sum(probs * grad_probs, axis=-1, keepdims=True))
    rounded = grad_scores.astype(jnp.bfloat16)
    grad_query = (
        jnp.einsum("hqk,khd->qhd", rounded, keys, preferred_element_type=jnp.float32) * factor
    )
    grad_keys = (
        jnp.einsum("hqk,qhd->khd", rounded, query, preferred_element_type=jnp.float32) * factor
    )
    grad_values = jnp.einsum(
        "hqk,qhd->khd", probs.astype(jnp.bfloat16), grad_mixed, preferred_element_type=jnp.float32
    )
    return (
        grad_query.astype(jnp.bfloat16),
        grad_keys.astype(jnp.bfloat16),
        grad_values.astype(jnp.bfloat16),
    )


def squared_total(grads, tensor_count):
    total = jnp.zeros((), jnp.float32)
    for incoming_gradient, shared in zip(grads, shared_terms):
        weight = 1.0 / tensor_count if shared else 1.0
        total = total + weight * jnp.sum(incoming_gradient * incoming_gradient)
    return total


def adam_step(master, row_mean, square, incoming_gradient, rate):
    mean_new = 0.5 * row_mean + 0.5 * incoming_gradient
    square_new = 0.5 * square + 0.5 * incoming_gradient * incoming_gradient
    change = -rate * (mean_new / (jnp.sqrt(square_new) + 1e-08) + 0.1 * master)
    updated = master + change
    return [updated, mean_new, square_new, updated.astype(jnp.bfloat16)]


def per_device(
    images,
    valid_flags,
    cotangent,
    first_gain,
    first_shift,
    triple_weight,
    pair_bias,
    output_weight,
    output_bias,
    second_gain,
    second_shift,
    expand_weight,
    expand_bias,
    reduce_weight,
    reduce_bias,
    first_gain_mean,
    first_shift_mean,
    triple_weight_mean,
    pair_bias_mean,
    output_weight_mean,
    output_bias_mean,
    second_gain_mean,
    second_shift_mean,
    expand_weight_mean,
    expand_bias_mean,
    reduce_weight_mean,
    reduce_bias_mean,
    first_gain_square,
    first_shift_square,
    triple_weight_square,
    pair_bias_square,
    output_weight_square,
    output_bias_square,
    second_gain_square,
    second_shift_square,
    expand_weight_square,
    expand_bias_square,
    reduce_weight_square,
    reduce_bias_square,
):
    masters = (
        first_gain,
        first_shift,
        triple_weight,
        pair_bias,
        output_weight,
        output_bias,
        second_gain,
        second_shift,
        expand_weight,
        expand_bias,
        reduce_weight,
        reduce_bias,
    )
    means = (
        first_gain_mean,
        first_shift_mean,
        triple_weight_mean,
        pair_bias_mean,
        output_weight_mean,
        output_bias_mean,
        second_gain_mean,
        second_shift_mean,
        expand_weight_mean,
        expand_bias_mean,
        reduce_weight_mean,
        reduce_bias_mean,
    )
    squares = (
        first_gain_square,
        first_shift_square,
        triple_weight_square,
        pair_bias_square,
        output_weight_square,
        output_bias_square,
        second_gain_square,
        second_shift_square,
        expand_weight_square,
        expand_bias_square,
        reduce_weight_square,
        reduce_bias_square,
    )
    rounded = tuple((master.astype(jnp.bfloat16) for master in masters))
    (
        first_norm_gain,
        first_norm_bias,
        triple,
        pairs,
        out_weight,
        out_bias,
        second_norm_gain,
        second_norm_bias,
        up_weight,
        up_bias,
        down_weight,
        down_bias,
    ) = (
        lax.all_gather(rounded[0], "dp", axis=0, tiled=True),
        lax.all_gather(rounded[1], "dp", axis=0, tiled=True),
        lax.all_gather(rounded[2], "dp", axis=1, tiled=True),
        lax.all_gather(rounded[3], "dp", axis=2, tiled=True),
        lax.all_gather(rounded[4], "dp", axis=1, tiled=True),
        lax.all_gather(rounded[5], "dp", axis=0, tiled=True),
        lax.all_gather(rounded[6], "dp", axis=0, tiled=True),
        lax.all_gather(rounded[7], "dp", axis=0, tiled=True),
        lax.all_gather(rounded[8], "dp", axis=0, tiled=True),
        lax.all_gather(rounded[9], "dp", axis=1, tiled=True),
        lax.all_gather(rounded[10], "dp", axis=1, tiled=True),
        lax.all_gather(rounded[11], "dp", axis=0, tiled=True),
    )
    shape = images.shape
    count = shape[0] * shape[1]
    heads_local = pairs.shape[1]
    head_size = pairs.shape[2]
    split = (shape[0], shape[1], heads_local, head_size)
    tensor_count = lax.axis_size("tensor")
    input_row_block = images.reshape(count, shape[2]).astype(jnp.float32)
    first_normed_rows, first_standardized, first_inverse_deviation = apply_layer_norm(
        input_row_block, first_norm_gain, first_norm_bias
    )
    inputs_one = first_normed_rows.astype(jnp.bfloat16)
    projected = jnp.einsum("td,cde->cte", inputs_one, triple, preferred_element_type=jnp.float32)
    pair_flat = pairs.reshape(2, -1).astype(jnp.float32)
    query = (projected[0] + pair_flat[0]).astype(jnp.bfloat16).reshape(split)
    keys = projected[1].astype(jnp.bfloat16).reshape(split)
    values = (projected[2] + pair_flat[1]).astype(jnp.bfloat16).reshape(split)
    mixed, logsum = lax.map(image_forward, (query, keys, values))
    mixed_flat = mixed.reshape(count, -1)
    attn_part = jnp.dot(mixed_flat, out_weight, preferred_element_type=jnp.float32)
    middle_state = input_row_block + lax.psum(attn_part, "tensor") + out_bias.astype(jnp.float32)
    second_normed_rows, second_standardized, second_inverse_deviation = apply_layer_norm(
        middle_state, second_norm_gain, second_norm_bias
    )
    inputs_two = second_normed_rows.astype(jnp.bfloat16)
    hidden = jnp.dot(inputs_two, up_weight, preferred_element_type=jnp.float32) + up_bias.reshape(
        -1
    ).astype(jnp.float32)
    active_full, gelu_back = jax.vjp(exact_gelu, hidden)
    active = active_full.astype(jnp.bfloat16)
    mlp_part = jnp.dot(active, down_weight, preferred_element_type=jnp.float32)
    result = middle_state + lax.psum(mlp_part, "tensor") + down_bias.astype(jnp.float32)
    block_output = result.astype(jnp.bfloat16)
    output_gradient = (
        cotangent.astype(jnp.float32) * valid_flags.astype(jnp.float32)[:, None, None]
    ).reshape(count, -1)
    grad_low = output_gradient.astype(jnp.bfloat16)
    grad_down_bias = jnp.sum(output_gradient, axis=0)
    grad_down_weight = contract_rows(active, grad_low)
    grad_active = against(grad_low, down_weight)
    grad_hidden = gelu_back(grad_active)[0]
    grad_up_bias = jnp.sum(grad_hidden, axis=0).reshape(up_bias.shape)
    hidden_low = grad_hidden.astype(jnp.bfloat16)
    grad_up_weight = contract_rows(inputs_two, hidden_low)
    second_normed_gradient = lax.psum(against(hidden_low, up_weight), "tensor")
    second_gain_gradient = jnp.sum(second_normed_gradient * second_standardized, axis=0)
    grad_shift_two = jnp.sum(second_normed_gradient, axis=0)
    middle_gradient = output_gradient + layer_norm_backward(
        second_normed_gradient, second_standardized, second_inverse_deviation, second_norm_gain
    )
    grad_out_bias = jnp.sum(middle_gradient, axis=0)
    middle_low = middle_gradient.astype(jnp.bfloat16)
    grad_out_weight = contract_rows(mixed_flat, middle_low)
    grad_mixed = against(middle_low, out_weight).astype(jnp.bfloat16).reshape(split)
    grad_query, grad_keys, grad_values = lax.map(
        image_backward, (query, keys, values, logsum, grad_mixed)
    )
    stacked = jnp.stack(
        [
            grad_query.reshape(count, -1),
            grad_keys.reshape(count, -1),
            grad_values.reshape(count, -1),
        ]
    )
    grad_pairs = jnp.stack(
        [
            jnp.sum(stacked[0].astype(jnp.float32), axis=0),
            jnp.sum(stacked[2].astype(jnp.float32), axis=0),
        ]
    ).reshape(pairs.shape)
    grad_triple = jnp.einsum("td,cte->cde", inputs_one, stacked, preferred_element_type=jnp.float32)
    back_one = jnp.einsum("cte,cde->td", stacked, triple, preferred_element_type=jnp.float32)
    first_normed_gradient = lax.psum(back_one, "tensor")
    first_gain_gradient = jnp.sum(first_normed_gradient * first_standardized, axis=0)
    grad_shift_one = jnp.sum(first_normed_gradient, axis=0)
    row_gradient = middle_gradient + layer_norm_backward(
        first_normed_gradient, first_standardized, first_inverse_deviation, first_norm_gain
    )
    grads = (
        first_gain_gradient,
        grad_shift_one,
        grad_triple,
        grad_pairs,
        grad_out_weight,
        grad_out_bias,
        second_gain_gradient,
        grad_shift_two,
        grad_up_weight,
        grad_up_bias,
        grad_down_weight,
        grad_down_bias,
    )
    summed = lax.psum(
        (
            grads[0],
            grads[1],
            grads[2],
            grads[3],
            grads[4],
            grads[5],
            grads[6],
            grads[7],
            grads[8],
            grads[9],
            grads[10],
            grads[11],
        ),
        "dp",
    )
    total = lax.psum(squared_total(summed, tensor_count), "tensor")
    position = lax.axis_index("dp")
    owned = tuple(
        (
            lax.dynamic_slice_in_dim(
                incoming_gradient, position * master.shape[dim], master.shape[dim], dim
            )
            for incoming_gradient, master, dim in zip(summed, masters, shard_dims)
        )
    )
    norm_value = jnp.sqrt(total)
    limit = math.sqrt(4 * D * D + 2 * D * FF + 8 * D + FF)
    factor = jnp.minimum(1.0, limit / (norm_value + 1e-06))
    updates = []
    for master, row_mean, square, incoming_gradient, rate in zip(
        masters, means, squares, owned, rates
    ):
        updates.extend(adam_step(master, row_mean, square, incoming_gradient * factor, rate))
    return (block_output.reshape(shape), row_gradient.reshape(shape), norm_value, *updates)


HEAD = 64
ROWS = 640
BLOCK = 160
SUB = 32
LANES = 128
BF = jnp.bfloat16
F32 = jnp.float32
NEG = -1e30
MESH = pl.DeviceIdType.MESH


def flip(index, pattern, bits):
    out = index
    for bit in range(bits):
        if (pattern >> bit) & 1:
            step = 1 << bit
            out = out + (1 - 2 * lax.rem(lax.div(index, step), 2)) * step
    return out


def nt(left, right):
    return lax.dot_general(left, right, (((1,), (1,)), ((), ())), preferred_element_type=F32)


def nn(left, right):
    return jnp.dot(left, right, preferred_element_type=F32)


def tile(index, size):
    if isinstance(index, int):
        return pl.ds(index * size, size)
    return pl.ds(pl.multiple_of(index * size, size), size)


def rows32(start, size):
    if isinstance(start, int):
        return pl.ds(start, size)
    return pl.ds(pl.multiple_of(start, SUB), size)


def center_scale(v):
    c = v - jnp.mean(v, axis=-1, keepdims=True)
    r = lax.rsqrt(jnp.mean(c * c, axis=-1, keepdims=True) + 1e-06)
    return c * r, r


SCRATCH = dict(
    xs=((ROWS, D), BF),
    gyb=((ROWS, D), BF),
    small_own=((8, LANES), F32),
    vec=((8, D), F32),
    vecb=((8, D), F32),
    bias3=((3, 1, 256), F32),
    ebias=((1, D), F32),
    wqkv=((3, D, 256), BF),
    wof=((D, D), BF),
    wr=((D, D), BF),
    we=((D, D), BF),
    a1=((ROWS, D), BF),
    a1t=((D, ROWS), BF),
    tt=((D, ROWS), BF),
    qkv=((3, ROWS, 256), BF),
    kt=((256, ROWS), BF),
    vt=((256, ROWS), BF),
    ot=((256, ROWS), BF),
    of=((ROWS, D), BF),
    lse=((4, 1, ROWS), F32),
    x1=((ROWS, D), F32),
    a2=((ROWS, D), BF),
    du=((ROWS, D), F32),
    hb=((ROWS, 256), F32),
    u=((ROWS, D), BF),
    dhb=((ROWS, D), BF),
    rs=((3, 3, BLOCK, D), BF),
    rout=((3, 3, BLOCK, D), BF),
    rin=((3, 2, BLOCK, D), BF),
    dxb=((256, D), BF),
    ott=((D, 256), BF),
    dobs=((3, BLOCK, 256), BF),
    dob=((ROWS, 256), BF),
    ds4=((ROWS, 512), BF),
    p4=((ROWS, 512), BF),
    qm4=((512, 256), BF),
    dm4=((512, 256), BF),
    dk=((ROWS, 256), F32),
    dv=((ROWS, 256), F32),
    dqt=((256, LANES), F32),
    dqkv=((3, ROWS, 256), BF),
    yb=((ROWS, D), BF),
    xg=((ROWS, D), BF),
    gwr=((D, D), BF),
    gwe=((D, D), BF),
    gwo=((D, D), BF),
    gwq=((3, D, 256), BF),
    pr_r=((4, D, LANES), BF),
    pr_e=((4, LANES, D), BF),
    pr_o=((4, D, LANES), BF),
    pr_q=((4, 3, LANES, 256), BF),
    cr_r=((3, D, LANES), BF),
    cr_e=((3, LANES, D), BF),
    cr_o=((3, D, LANES), BF),
    go_sum=((D, LANES), F32),
    goz=((D, LANES), BF),
    gor=((3, 256, LANES), BF),
    cr_q=((3, 3, LANES, 256), BF),
    sg=((8, D), F32),
    sgz=((3, 8, D), F32),
    sgt=((8, D), F32),
    sgd=((7, 8, D), F32),
    nrm=((2, 8, LANES), F32),
    nrz=((3, 8, LANES), F32),
    nrd=((7, 8, LANES), F32),
)
SEMS = dict(
    ld=(8,),
    g_s=(5, 8),
    g_r=(5, 8),
    wz_s=(3,),
    wz_r=(3,),
    o_s=(5, 5),
    o_r=(5, 4),
    z_s=(4, 3),
    z_r=(4, 3),
    rs_s=(3, 3),
    ro_r=(3, 3),
    ri_r=(3, 2),
    ag_s=(2, 5),
    ag_r=(2, 4),
    p_s=(4, 4),
    p_r=(4, 4),
    c_s=(4, 3),
    c_r=(4, 3),
    d_s=(2, 7),
    d_r=(2, 7),
)
INPUTS = dict(x_in=0, gy_in=0, small_in=0, q_in=0, o_in=0, e_in=0, r_in=0)
OUTPUTS = dict(gq=0, go=0, ge=0, gr=0, sg_out=0, total=0, y_out=0, xg_out=0)


def block_kernel(tokens, *refs):
    names = (*INPUTS, *OUTPUTS, *SCRATCH, *SEMS)
    R = types.SimpleNamespace(**dict(zip(names, refs)))
    me = lax.axis_index("dp")
    z = lax.axis_index("tensor")
    dpx = [flip(me, e, 3) for e in range(8)]
    zx = [flip(z, d, 2) for d in range(4)]
    half = lax.div(z, 2)
    near = z + half * (3 - 2 * z)
    inner = z + 1 - 2 * half
    outer = z - 1 + 2 * half
    at_end = near == 0
    at_middle = near == 1

    def seen(j):
        return j + half * (3 - 2 * j)

    order = (seen(3), seen(2), seen(1 - near), z)
    sent = []

    def remote(src, dst, send, recv, where):
        return pltpu.make_async_remote_copy(
            src_ref=src, dst_ref=dst, send_sem=send, recv_sem=recv,
            device_id=where, device_id_type=MESH,
        )

    def post(copy):
        copy.start()
        sent.append(copy)

    barrier = pltpu.get_barrier_semaphore()
    for e in range(1, 8):
        pl.semaphore_signal(barrier, inc=1, device_id={"dp": dpx[e]}, device_id_type=MESH)
    for d in range(1, 4):
        pl.semaphore_signal(barrier, inc=1, device_id={"tensor": zx[d]}, device_id_type=MESH)
    loads = [
        pltpu.make_async_copy(a, b, R.ld.at[i])
        for i, (a, b) in enumerate(
            (
                (R.small_in, R.small_own),
                (R.q_in, R.gq),
                (R.o_in, R.go),
                (R.r_in, R.gr),
                (R.e_in, R.ge),
                (R.x_in, R.xs),
                (R.gy_in, R.gyb),
            )
        )
    ]
    for copy in loads:
        copy.start()

    GATHER = {
        "small": (0, lambda j: R.vec.at[:, tile(j, LANES)]),
        "q": (1, lambda j: R.wqkv.at[:, tile(j, LANES), :]),
        "o": (2, lambda j: R.wof.at[:, tile(j, LANES)]),
        "r": (3, lambda j: R.wr.at[:, tile(j, LANES)]),
        "e": (4, lambda j: R.we.at[tile(j, LANES), :]),
    }

    HALF = {
        "o": lambda j, part: R.wof.at[tile(part, D // 2), tile(j, LANES)],
        "r": lambda j, part: R.wr.at[tile(part, D // 2), tile(j, LANES)],
        "e": lambda j, part: R.we.at[tile(2 * j + part, LANES // 2), :],
    }

    def gather_copy(name, source, target, slot, part=None):
        a, region = GATHER[name]
        piece = region(dpx[source]) if part is None else HALF[name](dpx[source], part)
        return remote(piece, piece, R.g_s.at[a, slot], R.g_r.at[a, slot], {"dp": dpx[target]})

    gathered = []

    def gather_post(*where):
        gather_copy(*where).start()
        gathered.append(where)

    def gather_send(name, targets=(6, 2, 4, 1)):
        for e in targets:
            gather_post(name, 0, e, e)

    def gather_pass(name):
        for e in (2, 4, 6):
            gather_copy(name, e, e, e).wait_recv()
            gather_post(name, e, 1, e + 1)

    def gather_relay(name):
        gather_copy(name, 2, 2, 2).wait_recv()
        gather_post(name, 2, 4, 6, 0)
        gather_copy(name, 4, 4, 4).wait_recv()
        gather_post(name, 4, 2, 0, 1)
        gather_post(name, 2, 1, 3)
        gather_post(name, 4, 1, 5)

    def gather_last(name):
        gather_copy(name, 6, 4, 6, 0).wait_recv()
        gather_copy(name, 6, 2, 0, 1).wait_recv()
        gather_post(name, 6, 1, 7)

    def gather_wait(name):
        for e in (1, 3, 5, 7):
            gather_copy(name, e, 1, e).wait_recv()

    def to_inner(src, dst, send, recv):
        return remote(src, dst, send, recv, {"tensor": inner})

    def to_outer(src, dst, send, recv):
        return remote(src, dst, send, recv, {"tensor": outer})

    def add_into(x, k, other, slot):
        @pl.loop(0, BLOCK // SUB)
        def _(i):
            rows = tile(i, SUB)
            total = R.rs[x, k, rows, :].astype(F32) + other[x, slot, rows, :].astype(F32)
            R.rs[x, k, rows, :] = total.astype(BF)

    class Scatter:
        def __init__(self, x):
            self.x = x

        def inward(self, k, dst, recv):
            return to_inner(R.rs.at[self.x, k], dst, R.rs_s.at[self.x, k], recv)

        def from_end(self, k):
            return self.inward(k, R.rout.at[self.x, k], R.ro_r.at[self.x, k])

        def across(self, k):
            return self.inward(k, R.rin.at[self.x, k], R.ri_r.at[self.x, k])

        def outward(self):
            return to_outer(
                R.rs.at[self.x, 2], R.rin.at[self.x, 0], R.rs_s.at[self.x, 2], R.ri_r.at[self.x, 0]
            )

        def end(self, k):
            @pl.when(at_end)
            def _():
                self.from_end(k).start()

        def step(self, k):
            @pl.when(at_middle)
            def _():
                if k < 2:
                    self.from_end(k).wait_recv()
                    add_into(self.x, k, R.rout, k)
                    self.across(k).start()
                else:
                    self.across(0).wait_recv()
                    add_into(self.x, 2, R.rin, 0)
                    self.outward().start()

        def finish(self, add):
            @pl.when(at_middle)
            def _():
                self.from_end(2).wait_recv()
                add(R.rout, self.x, 2)
                self.across(1).wait_recv()
                add(R.rin, self.x, 1)

            @pl.when(at_end)
            def _():
                self.across(0).wait_recv()
                add(R.rin, self.x, 0)

        def drain(self):
            for k in range(3):
                self.from_end(k).wait_send()

    class Spread:
        def __init__(self, region, sends, recvs, x):
            self.region, self.sends, self.recvs, self.x = region, sends, recvs, x

        def inward(self, j, slot, recv):
            part = self.region(seen(j))
            return to_inner(part, part, self.sends.at[self.x, slot], self.recvs.at[self.x, recv])

        def outward(self, j, slot, recv):
            part = self.region(seen(j))
            return to_outer(part, part, self.sends.at[self.x, slot], self.recvs.at[self.x, recv])

        def start(self):
            @pl.when(at_end)
            def _():
                self.inward(0, 0, 0).start()

            @pl.when(at_middle)
            def _():
                self.inward(1, 0, 2).start()
                self.outward(1, 1, 1).start()

        def first(self):
            @pl.when(at_middle)
            def _():
                self.outward(0, 2, 0).wait_recv()
                self.inward(0, 2, 3).start()
                self.inward(2, 3, 2).wait_recv()
                self.outward(2, 3, 2).start()

        def second(self):
            @pl.when(at_middle)
            def _():
                self.inward(3, 4, 3).wait_recv()
                self.outward(3, 4, 3).start()

        def finish(self):
            @pl.when(at_end)
            def _():
                for j in (1, 2, 3):
                    self.inward(j, 0, j).wait_recv()

        def drain(self):
            self.inward(0, 0, 0).wait_send()

            @pl.when(at_middle)
            def _():
                for slot in (1, 2, 3, 4):
                    self.inward(1, slot, 0).wait_send()

    own = tile(me, LANES)
    loads[0].wait()
    R.vec[:, own] = R.small_own[...]
    loads[1].wait()
    R.wqkv[:, own, :] = R.gq[...].astype(BF)
    loads[2].wait()
    R.wof[tile(z, 256), own] = R.go[...].astype(BF)
    pl.semaphore_wait(barrier, 10)
    gather_send("small")
    gather_send("q")
    for d in (3, 2, 1):
        part = R.wof.at[tile(z, 256), own]
        post(remote(part, part, R.wz_s.at[d - 1], R.wz_r.at[d - 1], {"tensor": zx[d]}))
    loads[3].wait()
    R.wr[:, own] = R.gr[...].astype(BF)
    loads[4].wait()
    R.we[own, :] = R.ge[...].astype(BF)
    for d in (1, 2, 3):
        part = R.wof.at[tile(zx[d], 256), own]
        remote(part, part, R.wz_s.at[d - 1], R.wz_r.at[d - 1], {"tensor": zx[d]}).wait_recv()
    gather_send("o", (2, 4, 1))

    gather_pass("small")
    gather_wait("small")
    R.vecb[...] = R.vec[...].astype(BF).astype(F32)
    spread_row = lax.broadcasted_iota(jnp.int32, (LANES, D), 0)
    spread_col = lax.broadcasted_iota(jnp.int32, (LANES, D), 1)
    spread = jnp.where(
        (lax.div(spread_row, 8) == lax.div(spread_col, 64))
        & (lax.rem(spread_row, 8) == lax.rem(spread_col, 8)),
        1.0,
        0.0,
    ).astype(BF)
    turn = lax.rem(lax.div(lax.broadcasted_iota(jnp.int32, (8, D), 1), 8), 8)
    pick = turn == lax.broadcasted_iota(jnp.int32, (8, D), 0)

    def unpack(row):
        parts = jnp.concatenate(
            [R.vecb[row : row + 1, j * LANES : (j + 1) * LANES] for j in range(8)], axis=0
        ).astype(BF)
        wide = nn(parts, spread)
        return jnp.sum(jnp.where(pick, wide, 0.0), axis=0, keepdims=True)

    R.ebias[...] = unpack(6)
    pair = unpack(7)
    R.bias3[0] = pair[:, :256]
    R.bias3[1] = jnp.zeros((1, 256), F32)
    R.bias3[2] = pair[:, 256:512]

    loads[5].wait()
    gain1, shift1 = R.vecb[0:1, :], R.vecb[1:2, :]
    sub_iota = lax.broadcasted_iota(jnp.int32, (SUB, 1), 0)

    @pl.loop(0, ROWS // SUB)
    def _(b):
        rows = tile(b, SUB)
        hat, _ = center_scale(R.xs[rows, :].astype(F32))
        out = jnp.where(sub_iota + b * SUB < tokens, hat * gain1 + shift1, 0.0)
        R.a1[rows, :] = out.astype(BF)

    def flip_into(target, source):
        @pl.loop(0, D // LANES)
        def _(i):
            target[tile(i, LANES), :] = source[:, tile(i, LANES)].T

    flip_into(R.a1t, R.a1)

    gather_pass("q")
    gather_send("r", (2, 4, 1))
    gather_wait("q")

    @pl.loop(0, 3)
    def _(c):
        acc = nn(R.a1[...], R.wqkv[c]) + R.bias3[c]
        R.qkv[c] = acc.astype(BF)

    scale = jnp.asarray(HEAD ** (-0.5), BF)
    R.qkv[0] = R.qkv[0] * scale
    R.kt[...] = R.qkv[1].T
    R.vt[...] = R.qkv[2].T
    head_lane = lax.div(lax.broadcasted_iota(jnp.int32, (LANES, 256), 1), HEAD)
    edge = tokens // 64 * 64
    tail_iota = lax.broadcasted_iota(jnp.int32, (ROWS - edge, LANES), 0) + edge

    def masked_scores(query):
        s = nt(R.qkv[1], query)
        return jnp.concatenate([s[:edge], jnp.where(tail_iota < tokens, s[edge:], NEG)], axis=0)

    def only_head(value, h):
        return jnp.where(head_lane == h, value, jnp.zeros_like(value))

    def o_spread(b):
        return Spread(lambda j: R.of.at[tile(b, LANES), tile(j, 256)], R.o_s, R.o_r, b)

    blocks = ROWS // LANES

    @pl.loop(0, ROWS // LANES)
    def _(b):
        cols = tile(b, LANES)
        query = R.qkv[0, cols, :]
        for h in range(4):
            s = masked_scores(only_head(query, h))
            top = jnp.max(s, axis=0, keepdims=True)
            p = jnp.exp(s - top)
            total = jnp.sum(p, axis=0, keepdims=True)
            R.lse[h, :, cols] = top + jnp.log(total)
            pb = (p * (1.0 / total)).astype(BF)
            mixed = nn(R.vt[h * HEAD : (h + 1) * HEAD, :], pb)
            R.ot[h * HEAD : (h + 1) * HEAD, cols] = mixed.astype(BF)
        R.of[cols, tile(z, 256)] = R.ot[:, cols].T
        o_spread(b).start()

        @pl.when(b >= 1)
        def _():
            o_spread(b - 1).first()

        @pl.when(b >= 2)
        def _():
            o_spread(b - 2).second()

        @pl.when(b == 1)
        def _():
            gather_relay("o")
            gather_send("e", (2, 4, 1))

    o_spread(blocks - 1).first()
    o_spread(blocks - 2).second()
    loads[6].wait()
    gather_last("o")
    gather_relay("r")
    o_spread(blocks - 1).second()
    gather_wait("o")

    out_bias = R.vecb[2:3, :]
    gain2, shift2 = R.vecb[3:4, :], R.vecb[4:5, :]

    @pl.loop(0, ROWS // LANES)
    def _(b):
        rows = tile(b, LANES)
        o_spread(b).finish()

        @pl.loop(0, 4)
        def _(n):
            cols = tile(n, 256)
            R.x1[rows, cols] = R.xs[rows, cols].astype(F32) + nn(R.of[rows, :], R.wof[:, cols])

        @pl.loop(0, LANES // SUB)
        def _(i):
            part = rows32(b * LANES + i * SUB, SUB)
            v = R.x1[part, :] + out_bias
            R.x1[part, :] = v
            hat, _ = center_scale(v)
            R.a2[part, :] = (hat * gain2 + shift2).astype(BF)

    gather_last("r")
    gather_relay("e")
    gather_wait("r")

    @pl.loop(0, 4)
    def _(n):
        R.du[:, tile(n, 256)] = nt(R.gyb[...], R.wr[tile(n, 256), :])

    gather_last("e")
    gather_wait("e")

    @pl.loop(0, 4)
    def _(n):
        cols = tile(n, 256)
        R.hb[...] = nn(R.a2[...], R.we[:, cols]) + R.ebias[:, cols]

        def part(i, total):
            rows = tile(i, SUB)
            h = R.hb[rows, :]
            cdf = 0.5 * (1.0 + lax.erf(h * math.sqrt(0.5)))
            slope = cdf + h * (jnp.exp(-0.5 * h * h) * (1.0 / math.sqrt(2.0 * math.pi)))
            dh = R.du[rows, cols] * slope
            R.u[rows, cols] = (h * cdf).astype(BF)
            R.dhb[rows, cols] = dh.astype(BF)
            return total + jnp.sum(dh, axis=0, keepdims=True)

        R.sg[6:7, cols] = lax.fori_loop(0, ROWS // SUB, part, jnp.zeros((1, 256), F32))

    def z_copy(x, d, src, dst):
        return remote(src, dst, R.z_s.at[x, d - 1], R.z_r.at[x, d - 1], {"tensor": zx[d]})

    scatter3, scatter2, scatter4 = Scatter(0), Scatter(1), Scatter(2)
    for k in range(4):
        rows = rows32(order[k] * BLOCK, BLOCK)

        @pl.loop(0, 4)
        def _(n):
            cols = tile(n, 256)
            part = nt(R.dhb[rows, :], R.we[cols, :])
            if k < 3:
                R.rs[0, k, :, cols] = part.astype(BF)
            else:
                R.du[0:BLOCK, cols] = part

        if k < 3:
            scatter3.end(k)

    PIECES = {
        "r": (0, R.pr_r, R.cr_r, R.gr, lambda j: R.gwr.at[:, tile(j, LANES)]),
        "e": (1, R.pr_e, R.cr_e, R.ge, lambda j: R.gwe.at[tile(j, LANES), :]),
        "o": (2, R.pr_o, R.cr_o, R.go_sum, lambda j: R.gwo.at[:, tile(j, LANES)]),
        "q": (3, R.pr_q, R.cr_q, R.gq, lambda j: R.gwq.at[:, tile(j, LANES), :]),
    }

    def pair_copy(name, t):
        a, pr, _, _, piece = PIECES[name]
        return remote(
            piece(dpx[2 * t + 1]), pr.at[t], R.p_s.at[a, t], R.p_r.at[a, t], {"dp": dpx[1]}
        )

    def cross_copy(name, t):
        a, _, cr, _, piece = PIECES[name]
        return remote(
            piece(dpx[2 * t]), cr.at[t - 1], R.c_s.at[a, t - 1], R.c_r.at[a, t - 1],
            {"dp": dpx[2 * t]},
        )

    def pair_send(name):
        for t in (3, 1, 2, 0):
            post(pair_copy(name, t))

    def pair_sum(name):
        _, pr, _, out, piece = PIECES[name]
        for t in (3, 1, 2, 0):
            pair_copy(name, t).wait_recv()
            held = piece(dpx[2 * t])
            both = held[...].astype(F32) + pr[t].astype(F32)
            if t:
                held[...] = both.astype(BF)
                post(cross_copy(name, t))
            else:
                out[...] = both

    def cross_sum(name):
        _, _, cr, out, _ = PIECES[name]
        for t in (1, 2, 3):
            cross_copy(name, t).wait_recv()
        both = out[...] + cr[0].astype(F32) + cr[1].astype(F32) + cr[2].astype(F32)
        out[...] = both
        return jnp.sum(both * both)

    flip_into(R.tt, R.u)

    @pl.loop(0, 4)
    def _(n):
        R.gwr[:, tile(n, 256)] = nn(R.tt[...], R.gyb[:, tile(n, 256)]).astype(BF)

    pair_send("r")
    flip_into(R.tt, R.a2)

    @pl.loop(0, 4)
    def _(n):
        R.gwe[:, tile(n, 256)] = nn(R.tt[...], R.dhb[:, tile(n, 256)]).astype(BF)

    pair_send("e")
    scatter3.step(0)
    pair_sum("r")

    for k in range(4):
        rows = rows32(order[k] * BLOCK, BLOCK)

        @pl.loop(0, 4)
        def _(n):
            cols = tile(n, 256)
            part = nn(R.u[rows, :], R.wr[:, cols])
            if k < 3:
                R.rs[1, k, :, cols] = part.astype(BF)
            else:
                R.du[BLOCK : 2 * BLOCK, cols] = part

    scatter3.step(1)
    pair_sum("e")
    scatter3.step(2)

    mine = z * BLOCK
    mine_rows = rows32(mine, BLOCK)

    def add_to(start):
        def add(other, x, slot):
            @pl.loop(0, BLOCK // SUB)
            def _(i):
                R.du[rows32(start + i * SUB, SUB), :] += other[x, slot, tile(i, SUB), :].astype(F32)

        return add

    scatter3.finish(add_to(0))

    def norm_part(i, sums):
        local = tile(i, SUB)
        rows = rows32(mine + i * SUB, SUB)
        dxn = R.du[local, :]
        hat, r = center_scale(R.x1[rows, :])
        gy = R.gyb[rows, :].astype(F32)
        e = dxn * gain2
        dx = gy + r * (
            e
            - jnp.mean(e, axis=-1, keepdims=True)
            - hat * jnp.mean(e * hat, axis=-1, keepdims=True)
        )
        R.du[rows32(3 * BLOCK + i * SUB, SUB), :] = dx
        R.dxb[local, :] = dx.astype(BF)
        terms = (dxn * hat, dxn, dx, gy)
        return tuple(s + jnp.sum(t, axis=0, keepdims=True) for s, t in zip(sums, terms))

    nothing = jnp.zeros((1, D), F32)
    sums = lax.fori_loop(0, BLOCK // SUB, norm_part, (nothing,) * 4)
    R.sg[3:4, :] = sums[0]
    R.sg[4:5, :] = sums[1]
    R.sg[2:3, :] = sums[2]
    R.sg[5:6, :] = sums[3]

    def dob_copy(d):
        return z_copy(0, d, R.dobs.at[d - 1], R.dob.at[mine_rows, :])

    for d in (3, 2, 1, 0):
        part = nt(R.dxb[0:BLOCK, :], R.wof[tile(zx[d], 256), :]).astype(BF)
        if d:
            R.dobs[d - 1] = part
            post(dob_copy(d))
        else:
            R.dob[mine_rows, :] = part

    for k in range(3):
        scatter2.end(k)

    R.dxb[BLOCK:, :] = jnp.zeros((256 - BLOCK, D), BF)
    R.ott[:, 128:] = jnp.zeros((D, 128), BF)

    @pl.loop(0, D // LANES)
    def _(i):
        R.ott[tile(i, LANES), 0:BLOCK] = R.of[mine_rows, tile(i, LANES)].T

    @pl.loop(0, 4)
    def _(n):
        R.gwo[:, tile(n, 256)] = nn(R.ott[...], R.dxb[:, tile(n, 256)]).astype(BF)

    pair_send("o")

    for d in (1, 2, 3):
        z_copy(0, d, R.dobs.at[d - 1], R.dob.at[rows32(zx[d] * BLOCK, BLOCK), :]).wait_recv()
    R.dk[...] = jnp.zeros_like(R.dk)
    R.dv[...] = jnp.zeros_like(R.dv)
    down_bias = R.vecb[5:6, :]

    @pl.loop(0, ROWS // LANES)
    def _(b):
        cols = tile(b, LANES)
        query = R.qkv[0, cols, :]
        grad = R.dob[cols, :]
        for h in range(4):
            lanes = slice(h * LANES, (h + 1) * LANES)
            qm = only_head(query, h)
            dm = only_head(grad, h)
            R.qm4[lanes, :] = qm
            R.dm4[lanes, :] = dm
            p = jnp.exp(masked_scores(qm) - R.lse[h, :, cols])
            R.p4[:, lanes] = p.astype(BF)
            dp = nt(R.qkv[2], dm)
            ds = (p * (dp - jnp.sum(p * dp, axis=0, keepdims=True))).astype(BF)
            R.ds4[:, lanes] = ds
            R.dqt[h * HEAD : (h + 1) * HEAD, :] = nn(R.kt[h * HEAD : (h + 1) * HEAD, :], ds)
        R.dqkv[0, cols, :] = (R.dqt[...].T * HEAD ** (-0.5)).astype(BF)
        R.dk[...] += nn(R.ds4[...], R.qm4[...])
        R.dv[...] += nn(R.p4[...], R.dm4[...])

    R.dqkv[1] = R.dk[...].astype(BF)
    R.dqkv[2] = R.dv[...].astype(BF)

    for k in range(3):
        scatter2.step(k)

    R.sg[7:8, :] = jnp.concatenate(
        [
            jnp.sum(R.dqkv[0].astype(F32), axis=0, keepdims=True),
            jnp.sum(R.dqkv[2].astype(F32), axis=0, keepdims=True),
            jnp.zeros((1, 512), F32),
        ],
        axis=1,
    )
    R.sg[0:2, :] = jnp.zeros((2, D), F32)
    for k in range(4):
        start = order[k] * BLOCK
        rows = rows32(start, BLOCK)

        @pl.loop(0, 4)
        def _(n):
            cols = tile(n, 256)
            R.du[0:BLOCK, cols] = (
                nt(R.dqkv[0, rows, :], R.wqkv[0, cols, :])
                + nt(R.dqkv[1, rows, :], R.wqkv[1, cols, :])
                + nt(R.dqkv[2, rows, :], R.wqkv[2, cols, :])
            )

        def first_part(i, sums):
            local = tile(i, SUB)
            dxn = R.du[local, :]
            hat, _ = center_scale(R.xs[rows32(start + i * SUB, SUB), :].astype(F32))
            if k < 3:
                R.rs[2, k, local, :] = dxn.astype(BF)
            terms = (dxn * hat, dxn)
            return tuple(s + jnp.sum(t, axis=0, keepdims=True) for s, t in zip(sums, terms))

        sums = lax.fori_loop(0, BLOCK // SUB, first_part, (nothing,) * 2)
        R.sg[0:1, :] += sums[0]
        R.sg[1:2, :] += sums[1]
        if k < 3:
            scatter4.end(k)

    for d in (3, 2, 1):
        post(z_copy(1, d, R.sg, R.sgz.at[d - 1]))

    @pl.loop(0, 3)
    def _(c):
        R.gwq[c] = nn(R.a1t[...], R.dqkv[c]).astype(BF)

    pair_send("q")
    pair_sum("o")
    scatter4.step(0)

    scatter2.finish(add_to(BLOCK))

    @pl.loop(0, BLOCK // SUB)
    def _(i):
        rows = rows32(mine + i * SUB, SUB)
        y = R.x1[rows, :] + R.du[rows32(BLOCK + i * SUB, SUB), :] + down_bias
        R.yb[rows, :] = y.astype(BF)

    y_spread = Spread(
        lambda j: R.yb.at[rows32(j * BLOCK, BLOCK), :], R.ag_s, R.ag_r, 0
    )
    x_spread = Spread(
        lambda j: R.xg.at[rows32(j * BLOCK, BLOCK), :], R.ag_s, R.ag_r, 1
    )
    y_spread.start()
    pair_sum("q")
    scatter4.step(1)
    squares = cross_sum("r")
    y_spread.first()
    scatter4.step(2)
    squares += cross_sum("e")
    y_spread.second()

    for d in (1, 2, 3):
        z_copy(1, d, R.sg, R.sgz.at[d - 1]).wait_recv()
    shared_row = lax.broadcasted_iota(jnp.int32, (8, D), 0) < 6
    others = R.sgz[0] + R.sgz[1] + R.sgz[2]
    R.sgt[...] = R.sg[...] + jnp.where(shared_row, others, 0.0)

    def d_copy(x, e, src, dst):
        return remote(src, dst, R.d_s.at[x, e - 1], R.d_r.at[x, e - 1], {"dp": dpx[e]})

    for e in (6, 7, 2, 3, 4, 5, 1):
        post(d_copy(0, e, R.sgt, R.sgd.at[e - 1]))

    scatter4.finish(add_to(0))

    @pl.loop(0, BLOCK // SUB)
    def _(i):
        local = tile(i, SUB)
        rows = rows32(mine + i * SUB, SUB)
        dxn = R.du[local, :]
        hat, r = center_scale(R.xs[rows, :].astype(F32))
        e = dxn * gain1
        dx = R.du[rows32(3 * BLOCK + i * SUB, SUB), :] + r * (
            e
            - jnp.mean(e, axis=-1, keepdims=True)
            - hat * jnp.mean(e * hat, axis=-1, keepdims=True)
        )
        R.xg[rows, :] = dx.astype(BF)

    x_spread.start()

    cross_sum("o")
    R.goz[...] = R.go_sum[...].astype(BF)
    for d in (3, 2, 1):
        post(z_copy(3, d, R.goz.at[tile(zx[d], 256), :], R.gor.at[d - 1]))
    squares += cross_sum("q")
    x_spread.first()
    for e in range(1, 8):
        d_copy(0, e, R.sgt, R.sgd.at[e - 1]).wait_recv()
    x_spread.second()
    for d in (1, 2, 3):
        z_copy(3, d, R.goz.at[tile(zx[d], 256), :], R.gor.at[d - 1]).wait_recv()
    own_out = (
        R.go_sum[tile(z, 256), :]
        + R.gor[0].astype(F32)
        + R.gor[1].astype(F32)
        + R.gor[2].astype(F32)
    )
    R.go[...] = own_out
    squares += jnp.sum(own_out * own_out)
    sg = R.sgt[...]
    for e in range(1, 8):
        sg = sg + R.sgd[e - 1]
    R.sg_out[...] = sg
    squared = sg * sg
    shared_squares = jnp.sum(jnp.where(shared_row, squared, 0.0))
    local_squares = jnp.sum(jnp.where(shared_row, 0.0, squared))
    R.nrm[0] = jnp.full((8, LANES), squares + local_squares * 0.125, F32)
    for e in (6, 7, 2, 3, 4, 5, 1):
        post(d_copy(1, e, R.nrm.at[0], R.nrd.at[e - 1]))
    for e in range(1, 8):
        d_copy(1, e, R.nrm.at[0], R.nrd.at[e - 1]).wait_recv()
    value = R.nrm[0]
    for e in range(1, 8):
        value = value + R.nrd[e - 1]
    R.nrm[1] = value
    for d in (3, 2, 1):
        post(z_copy(2, d, R.nrm.at[1], R.nrz.at[d - 1]))

    y_spread.finish()
    y_store = pltpu.make_async_copy(R.yb, R.y_out, R.ld.at[0])
    y_store.start()
    x_spread.finish()
    x_store = pltpu.make_async_copy(R.xg, R.xg_out, R.ld.at[1])
    x_store.start()
    for d in (1, 2, 3):
        z_copy(2, d, R.nrm.at[1], R.nrz.at[d - 1]).wait_recv()
    R.total[...] = R.nrm[1] + R.nrz[0] + R.nrz[1] + R.nrz[2] + shared_squares
    for copy in sent:
        copy.wait_send()
    for where in gathered:
        gather_copy(*where).wait_send()

    @pl.loop(0, ROWS // LANES)
    def _(b):
        o_spread(b).drain()

    for flow in (scatter3, scatter2, scatter4, y_spread, x_spread):
        flow.drain()

    y_store.wait()
    x_store.wait()


def run_block(tokens, x_rows, gy_rows, small, triple, out, up, down):
    kernel = functools.partial(block_kernel, tokens)
    vmem = pl.BlockSpec(memory_space=pltpu.VMEM)
    anywhere = pl.BlockSpec(memory_space=pl.ANY)
    return pl.pallas_call(
        kernel,
        out_shape=(
            jax.ShapeDtypeStruct((3, LANES, 256), F32),
            jax.ShapeDtypeStruct((256, LANES), F32),
            jax.ShapeDtypeStruct((LANES, D), F32),
            jax.ShapeDtypeStruct((D, LANES), F32),
            jax.ShapeDtypeStruct((8, D), F32),
            jax.ShapeDtypeStruct((8, LANES), F32),
            jax.ShapeDtypeStruct((ROWS, D), BF),
            jax.ShapeDtypeStruct((ROWS, D), BF),
        ),
        in_specs=[anywhere] * len(INPUTS),
        out_specs=(vmem,) * 6 + (anywhere,) * 2,
        scratch_shapes=[
            *(pltpu.VMEM(shape, dtype) for shape, dtype in SCRATCH.values()),
            *(pltpu.SemaphoreType.DMA(shape) for shape in SEMS.values()),
        ],
        compiler_params=pltpu.CompilerParams(
            collective_id=0, has_side_effects=True, vmem_limit_bytes=63 * 1024 * 1024
        ),
        name="block_step",
    )(x_rows, gy_rows, small, triple, out, up, down)


def fused_device(*args):
    images, valid_flags, cotangent = args[:3]
    masters, means, squares = args[3:15], args[15:27], args[27:39]
    tokens = images.shape[1]
    pad = ((0, ROWS - tokens), (0, 0))
    x_rows = jnp.pad(images[0], pad)
    gy_rows = jnp.pad(cotangent[0] * valid_flags[0].astype(BF), pad)
    vectors = [masters[i].reshape(1, LANES) for i in (0, 1, 5, 6, 7, 11)]
    small = jnp.concatenate(
        [
            *vectors,
            masters[9].reshape(1, LANES),
            jnp.pad(masters[3].reshape(1, HEAD), ((0, 0), (0, LANES - HEAD))),
        ],
        axis=0,
    )
    gq, go, ge, gr, sg, total, y_rows, grad_rows = run_block(
        tokens, x_rows, gy_rows, small, masters[2], masters[4], masters[8], masters[10]
    )
    position = lax.axis_index("dp")
    owned = lax.dynamic_slice_in_dim(sg[:6], position * LANES, LANES, 1)
    expand = lax.dynamic_slice_in_dim(sg[6].reshape(16, 64), position * 8, 8, 1)
    pairs = lax.dynamic_slice_in_dim(sg[7, :512].reshape(2, 4, 64), position * 8, 8, 2)
    grads = (
        owned[0], owned[1], gq, pairs, go, owned[2], owned[3], owned[4], ge, expand, gr, owned[5],
    )
    norm_value = jnp.sqrt(total[0, 0])
    limit = math.sqrt(4 * D * D + 2 * D * FF + 8 * D + FF)
    factor = jnp.minimum(1.0, limit / (norm_value + 1e-06))
    updates = []
    for master, row_mean, square, gradient, rate in zip(masters, means, squares, grads, rates):
        updates.extend(adam_step(master, row_mean, square, gradient * factor, rate))
    return (
        y_rows[:tokens].reshape(images.shape),
        grad_rows[:tokens].astype(F32).reshape(images.shape),
        norm_value,
        *updates,
    )


def solution(mesh):
    in_specs = (
        P("dp", None, None),
        P("dp"),
        P("dp", None, None),
        P("dp"),
        P("dp"),
        P(None, "dp", "tensor"),
        P(None, "tensor", "dp"),
        P("tensor", "dp"),
        P("dp"),
        P("dp"),
        P("dp"),
        P("dp", "tensor"),
        P("tensor", "dp"),
        P("tensor", "dp"),
        P("dp"),
        P("dp"),
        P("dp"),
        P(None, "dp", "tensor"),
        P(None, "tensor", "dp"),
        P("tensor", "dp"),
        P("dp"),
        P("dp"),
        P("dp"),
        P("dp", "tensor"),
        P("tensor", "dp"),
        P("tensor", "dp"),
        P("dp"),
        P("dp"),
        P("dp"),
        P(None, "dp", "tensor"),
        P(None, "tensor", "dp"),
        P("tensor", "dp"),
        P("dp"),
        P("dp"),
        P("dp"),
        P("dp", "tensor"),
        P("tensor", "dp"),
        P("tensor", "dp"),
        P("dp"),
    )
    out_specs = (
        P("dp", None, None),
        P("dp", None, None),
        P(),
        P("dp"),
        P("dp"),
        P("dp"),
        P("dp"),
        P("dp"),
        P("dp"),
        P("dp"),
        P("dp"),
        P(None, "dp", "tensor"),
        P(None, "dp", "tensor"),
        P(None, "dp", "tensor"),
        P(None, "dp", "tensor"),
        P(None, "tensor", "dp"),
        P(None, "tensor", "dp"),
        P(None, "tensor", "dp"),
        P(None, "tensor", "dp"),
        P("tensor", "dp"),
        P("tensor", "dp"),
        P("tensor", "dp"),
        P("tensor", "dp"),
        P("dp"),
        P("dp"),
        P("dp"),
        P("dp"),
        P("dp"),
        P("dp"),
        P("dp"),
        P("dp"),
        P("dp"),
        P("dp"),
        P("dp"),
        P("dp"),
        P("dp", "tensor"),
        P("dp", "tensor"),
        P("dp", "tensor"),
        P("dp", "tensor"),
        P("tensor", "dp"),
        P("tensor", "dp"),
        P("tensor", "dp"),
        P("tensor", "dp"),
        P("tensor", "dp"),
        P("tensor", "dp"),
        P("tensor", "dp"),
        P("tensor", "dp"),
        P("dp"),
        P("dp"),
        P("dp"),
        P("dp"),
    )
    fused = mesh.shape["dp"] == 8 and mesh.shape["tensor"] == 4
    return jax.shard_map(
        fused_device if fused else per_device, mesh=mesh, in_specs=in_specs, out_specs=out_specs, check_vma=False
    )
```
